256 devices in a mesh: row: 32 (over z_lo, y, core), col: 8 (over x, z_hi).
Axes of the slice: x: 4, y: 4, z: 8 (z_hi: 2, z_lo: 4; z = z_hi * 4 + z_lo), core: 2. Of those that a mesh axis runs over, the one named last changes fastest.
Arguments:
- pair_rep: bfloat16 [2048, 2048, 128], P('row', 'col'), may hold values from -6 to 6
- bias_weight: bfloat16 [128, 12], replicated, may hold values from -0.5 to 0.5
- head_weight: float32 [12], replicated, may hold values from -1 to 1
- queries: float32 [192, 2048], P(None, 'row'), may hold values from -48 to 48, as said below
- key_vectors: float32 [192, 2048], P(None, 'col'), may hold values from -48 to 48, as said below
- values: float32 [192, 2048], P(None, 'col'), may hold values from -6 to 6
- query_points: float32 [3, 48, 2048], P(None, None, 'row'), may hold values from -6 to 6
- key_points: float32 [3, 48, 2048], P(None, None, 'col'), may hold values from -6 to 6
- value_points: float32 [3, 96, 2048], P(None, None, 'col'), may hold values from -6 to 6
- rotations: float32 [3, 3, 2048], replicated, may hold values from -1 to 1, as said below
- translations: float32 [3, 2048], replicated, may hold values from -12 to 12
- residue_count: int32 [1], replicated, may hold values from 1024 to 2048
- grad_output: float32 [192, 2048], P(None, 'row'), may hold values from -6 to 6
- grad_points: float32 [3, 96, 2048], P(None, None, 'row'), may hold values from -6 to 6
- grad_pair: bfloat16 [2048, 12, 128], P('row'), may hold values from -2 to 2
Outputs:
- pair_grad: bfloat16 [2048, 2048, 128], P('row', 'col')
- query_grad: float32 [192, 2048], P(None, ('row', 'col'))
- query_point_grad: float32 [3, 48, 2048], P(None, None, ('row', 'col'))
- query_frame_grad: float32 [3, 4, 2048], P(None, None, ('row', 'col'))
- key_grad: float32 [192, 2048], P(None, ('col', 'row'))
- value_grad: float32 [192, 2048], P(None, ('col', 'row'))
- key_point_grad: float32 [3, 48, 2048], P(None, None, ('col', 'row'))
- value_point_grad: float32 [3, 96, 2048], P(None, None, ('col', 'row'))
- key_frame_grad: float32 [3, 4, 2048], P(None, None, ('col', 'row'))
- bias_weight_grad: float32 [128, 12], replicated
- head_weight_grad: float32 [12], replicated
The draws below stay inside these ranges and needn't reach their ends.
Inputs may be any that keep to these rules, and one draw needn't show every extreme that they name: `queries`: entries of order one, except a few residues whose vectors are much larger. `key_vectors`: entries of order one, except a few residues whose vectors are much larger. `rotations`: each residue's 3 x 3 matrix is a rotation: orthonormal with determinant one.
All inputs are finite; a program needn't handle non-finite values.
Results may differ from the reference program's by a relative error of at most 0.0049.
Values sent between devices are 32-bit elements; how exact they have to be, the bound alone decides.
A program may use at most 128 MiB of HBM per device.

```python
import math
import jax
import jax.numpy as jnp
from jax import lax

N = 2048
H = 12
C = 16
PQ = 4
PV = 8
CZ = 128


def drawn_vectors(key):
    base_key = jax.random.fold_in(key, 11)
    first, second = jax.random.split(base_key, 2)
    query_draw = jnp.clip(jax.random.normal(first, (H * C, N), jnp.float32), -4.0, 4.0)
    key_draw = jnp.clip(jax.random.normal(second, (H * C, N), jnp.float32), -4.0, 4.0)
    return (query_draw, key_draw)


def draw_queries(key, part):
    return drawn_vectors(key)[0]


def draw_key_vectors(key, part):
    return drawn_vectors(key)[1]


def draw_rotations(key, part):
    base_key = jax.random.fold_in(key, 23)
    first, second = jax.random.split(base_key)
    scalar = jax.random.uniform(first, (N,), jnp.float32, 0.5, 1.5)
    vector = jax.random.normal(second, (3, N), jnp.float32)
    length = jnp.sqrt(scalar ** 2 + jnp.sum(vector ** 2, axis=0))
    qw = scalar / length
    qx = vector[0] / length
    qy = vector[1] / length
    qz = vector[2] / length
    first_row = jnp.stack([1 - 2 * (qy * qy + qz * qz), 2 * (qx * qy - qw * qz), 2 * (qx * qz + qw * qy)])
    second_row = jnp.stack([2 * (qx * qy + qw * qz), 1 - 2 * (qx * qx + qz * qz), 2 * (qy * qz - qw * qx)])
    third_row = jnp.stack([2 * (qx * qz - qw * qy), 2 * (qy * qz + qw * qx), 1 - 2 * (qx * qx + qy * qy)])
    return jnp.stack([first_row, second_row, third_row])


def levels(stream_key, dims, shards, least, high):
    factor_of, own = 1.0, jax.random.fold_in(stream_key, 6)
    for position, parts in shards:
        heights = jnp.exp(jax.random.uniform(jax.random.fold_in(own, position), (parts,), jnp.float32, least / len(shards), high / len(shards)))
        factor_of = factor_of * jnp.repeat(heights, dims[position] // parts).reshape([-1 if axis == position else 1 for axis in range(len(dims))])
    return factor_of


def gaussian(own_key, shape, deviation, most, pieces=(), kind=jnp.bfloat16):
    loudness = levels(own_key, shape, pieces, -0.22, 0.18) if pieces else 1.0
    drawn = jax.random.normal(own_key, shape, jnp.float32) * deviation * loudness
    return jnp.minimum(jnp.maximum(drawn, -most), most).astype(kind)


def setup_inputs(seed: int = 0) -> dict:
    key_list = jax.random.split(jax.random.key(seed), 16)
    return {
        "pair_rep": gaussian(key_list[0], (N, N, CZ), 1.0, 6.0, ((0, 32), (1, 8))),
        "bias_weight": gaussian(key_list[1], (CZ, H), CZ ** -0.5, 0.5),
        "head_weight": jnp.clip(jax.random.uniform(key_list[2], (H,), jnp.float32, -1.0, 1.0), -1.0, 1.0),
        "queries": draw_queries(jax.random.fold_in(key_list[15], 71), 0),
        "key_vectors": draw_key_vectors(jax.random.fold_in(key_list[15], 71), 0),
        "values": gaussian(key_list[5], (H * C, N), 1.0, 6.0, ((1, 8),), jnp.float32),
        "query_points": gaussian(key_list[6], (3, H * PQ, N), 1.0, 6.0, ((2, 32),), jnp.float32),
        "key_points": gaussian(key_list[7], (3, H * PQ, N), 1.0, 6.0, ((2, 8),), jnp.float32),
        "value_points": gaussian(key_list[8], (3, H * PV, N), 1.0, 6.0, ((2, 8),), jnp.float32),
        "rotations": draw_rotations(jax.random.fold_in(key_list[15], 71), 0),
        "translations": gaussian(key_list[10], (3, N), 2.0, 12.0, (), jnp.float32),
        "residue_count": jax.random.randint(key_list[11], (1,), N // 2, N + 1).astype(jnp.int32),
        "grad_output": gaussian(key_list[12], (H * C, N), 1.0, 6.0, ((1, 32),), jnp.float32),
        "grad_points": gaussian(key_list[13], (3, H * PV, N), 1.0, 6.0, ((2, 32),), jnp.float32),
        "grad_pair": gaussian(key_list[14], (N, H, CZ), 0.3, 2.0, ((0, 32),)),
    }


HIGHEST = lax.Precision.HIGHEST

def globalize(rotation, offset, local):
    return jnp.einsum('xym,ykm->xkm', rotation, local, precision=HIGHEST) + offset[:, None, :]

def rotate_back(rotation, vector):
    return jnp.einsum('xym,xkm->ykm', rotation, vector, precision=HIGHEST)

def frame_terms(grad_global, local):
    rotation_part = jnp.einsum('xkm,ykm->xym', grad_global, local, precision=HIGHEST)
    return jnp.concatenate([rotation_part, lax.optimization_barrier(jnp.sum(grad_global, axis=1))[:, None, :]], axis=1)

def output_frame_terms(point_out, offset, cotan_local, grad_rotated):
    rotation_part = jnp.einsum('xkm,ykm->xym', point_out - offset[:, None, :], cotan_local, precision=HIGHEST)
    return jnp.concatenate([rotation_part, -lax.optimization_barrier(jnp.sum(grad_rotated, axis=1))[:, None, :]], axis=1)

def reference(pair_rep, bias_weight, head_weight, queries, key_vectors, values, query_points, key_points, value_points, rotations, translations, residue_count, grad_output, grad_points, grad_pair):
    logit_scale = math.sqrt(1.0 / 3.0)
    point_scale = math.sqrt(2.0 / (9.0 * PQ))
    inner_scale = 1.0 / math.sqrt(C)
    distance_coef = 0.5 * logit_scale * point_scale * jax.nn.softplus(head_weight)
    query_global = globalize(rotations, translations, query_points).reshape(3, H, PQ, N)
    key_global = globalize(rotations, translations, key_points).reshape(3, H, PQ, N)
    value_global = globalize(rotations, translations, value_points).reshape(3, H, PV, N)
    grad_global = jnp.einsum('xym,ykm->xkm', rotations, grad_points, precision=HIGHEST)
    grad_heads = grad_global.reshape(3, H, PV, N)
    key_heads = key_vectors.reshape(H, C, N)
    value_heads = values.reshape(H, C, N)
    query_heads = queries.reshape(H, C, N)
    out_heads = grad_output.reshape(H, C, N)
    valid = jnp.arange(N) < residue_count[0]
    pair_weight = bias_weight.astype(jnp.float32)
    block = min(128, N)

    def step(carry, start):
        pair_block = lax.dynamic_slice_in_dim(pair_rep, start, block, 0).astype(jnp.float32)
        cotan_pair = lax.dynamic_slice_in_dim(grad_pair, start, block, 0).astype(jnp.float32)
        query_block = lax.dynamic_slice_in_dim(query_heads, start, block, 2)
        out_block = lax.dynamic_slice_in_dim(out_heads, start, block, 2)
        qglobal_block = lax.dynamic_slice_in_dim(query_global, start, block, 3)
        gglobal_block = lax.dynamic_slice_in_dim(grad_heads, start, block, 3)
        inner = jnp.einsum('hci,hcj->hij', query_block, key_heads, precision=HIGHEST)
        cross = jnp.einsum('xhpi,xhpj->hij', qglobal_block, key_global, precision=HIGHEST)
        distance = lax.optimization_barrier(jnp.sum(qglobal_block ** 2, axis=(0, 2)))[:, :, None] + lax.optimization_barrier(jnp.sum(key_global ** 2, axis=(0, 2)))[:, None, :] - 2.0 * cross
        bias = jnp.einsum('ijc,ch->hij', pair_block, pair_weight, precision=HIGHEST)
        logits = logit_scale * (inner_scale * inner + bias) - distance_coef[:, None, None] * distance
        logits = jnp.where(valid[None, None, :], logits, jnp.float32(-1000000000.0))
        row_peak = lax.optimization_barrier(jnp.max(logits, axis=2, keepdims=True))
        exponent = jnp.exp(logits - row_peak)
        attention = exponent / lax.optimization_barrier(jnp.sum(exponent, axis=2, keepdims=True))
        product = jnp.einsum('hci,hcj->hij', out_block, value_heads, precision=HIGHEST) + jnp.einsum('xhvi,xhvj->hij', gglobal_block, value_global, precision=HIGHEST) + jnp.einsum('ijc,ihc->hij', pair_block, cotan_pair, precision=HIGHEST)
        delta = lax.optimization_barrier(jnp.sum(attention * product, axis=2, keepdims=True))
        logit_grad = attention * (product - delta)
        query_grad = logit_scale * inner_scale * jnp.einsum('hij,hcj->hci', logit_grad, key_heads, precision=HIGHEST)
        row_sum = lax.optimization_barrier(jnp.sum(logit_grad, axis=2))
        qpoint_grad = -2.0 * distance_coef[None, :, None, None] * (qglobal_block * row_sum[None, :, None, :] - jnp.einsum('hij,xhpj->xhpi', logit_grad, key_global, precision=HIGHEST))
        qpoint_flat = qpoint_grad.reshape(3, H * PQ, block)
        point_out = jnp.einsum('hij,xhvj->xhvi', attention, value_global, precision=HIGHEST).reshape(3, H * PV, block)
        rot_block = lax.dynamic_slice_in_dim(rotations, start, block, 2)
        shift_block = lax.dynamic_slice_in_dim(translations, start, block, 1)
        local_block = lax.dynamic_slice_in_dim(query_points, start, block, 2)
        cotan_local = lax.dynamic_slice_in_dim(grad_points, start, block, 2)
        gflat_block = gglobal_block.reshape(3, H * PV, block)
        qlocal_grad = rotate_back(rot_block, qpoint_flat)
        qframe = frame_terms(qpoint_flat, local_block) + output_frame_terms(point_out, shift_block, cotan_local, gflat_block)
        key_part = logit_scale * inner_scale * jnp.einsum('hij,hci->hcj', logit_grad, query_block, precision=HIGHEST)
        value_part = jnp.einsum('hij,hci->hcj', attention, out_block, precision=HIGHEST)
        col_sum = lax.optimization_barrier(jnp.sum(logit_grad, axis=1))
        kpoint_part = 2.0 * distance_coef[None, :, None, None] * (jnp.einsum('hij,xhpi->xhpj', logit_grad, qglobal_block, precision=HIGHEST) - key_global * col_sum[None, :, None, :])
        vpoint_part = jnp.einsum('hij,xhvi->xhvj', attention, gglobal_block, precision=HIGHEST)
        grad_rounded = lax.optimization_barrier(logit_grad.astype(jnp.bfloat16)).astype(jnp.float32)
        attn_rounded = lax.optimization_barrier(attention.astype(jnp.bfloat16)).astype(jnp.float32)
        weight_part = logit_scale * jnp.einsum('ijc,hij->ch', pair_block, grad_rounded, precision=HIGHEST)
        distance_part = lax.optimization_barrier(jnp.sum(logit_grad * distance, axis=(1, 2)))
        pair_grad = (logit_scale * jnp.einsum('hij,ch->ijc', grad_rounded, pair_weight, precision=HIGHEST) + jnp.einsum('hij,ihc->ijc', attn_rounded, cotan_pair, precision=HIGHEST)).astype(jnp.bfloat16)
        new_carry = (carry[0] + key_part, carry[1] + value_part, carry[2] + kpoint_part, carry[3] + vpoint_part, carry[4] + weight_part, carry[5] + distance_part)
        return (new_carry, (pair_grad, query_grad.reshape(H * C, block), qlocal_grad, qframe))
    initial = (jnp.zeros((H, C, N), jnp.float32), jnp.zeros((H, C, N), jnp.float32), jnp.zeros((3, H, PQ, N), jnp.float32), jnp.zeros((3, H, PV, N), jnp.float32), jnp.zeros((CZ, H), jnp.float32), jnp.zeros((H,), jnp.float32))
    starts = jnp.arange(N // block, dtype=jnp.int32) * block
    carry, stacked = lax.scan(step, initial, starts)
    pair_grad = stacked[0].reshape(N, N, CZ)
    query_grad = jnp.transpose(stacked[1], (1, 0, 2)).reshape(H * C, N)
    query_point_grad = jnp.transpose(stacked[2], (1, 2, 0, 3)).reshape(3, H * PQ, N)
    query_frame_grad = jnp.transpose(stacked[3], (1, 2, 0, 3)).reshape(3, 4, N)
    kpoint_flat = carry[2].reshape(3, H * PQ, N)
    vpoint_flat = carry[3].reshape(3, H * PV, N)
    key_point_grad = rotate_back(rotations, kpoint_flat)
    value_point_grad = rotate_back(rotations, vpoint_flat)
    key_frame_grad = frame_terms(kpoint_flat, key_points) + frame_terms(vpoint_flat, value_points)
    head_weight_grad = carry[5] * (-0.5 * logit_scale * point_scale) * jax.nn.sigmoid(head_weight)
    return (pair_grad, query_grad, query_point_grad, query_frame_grad, carry[0].reshape(H * C, N), carry[1].reshape(H * C, N), key_point_grad, value_point_grad, key_frame_grad, carry[4], head_weight_grad)
```

```python
import functools
import math

import jax
import jax.numpy as jnp
from jax import lax
from jax.experimental import pallas as pl
from jax.experimental.pallas import tpu as pltpu
from jax.sharding import Mesh
from jax.sharding import PartitionSpec as P

ROW = ("row_0", "row_1", "row_2")
COL = ("col_0", "col_1")
ROW_COL = ("row_0", "row_1", "row_2", "col_0", "col_1")
COL_ROW = ("col_0", "col_1", "row_0", "row_1", "row_2")

MESH = pl.DeviceIdType.MESH
HIGHEST = lax.Precision.HIGHEST
F32 = jnp.float32
BF16 = jnp.bfloat16
VMEM = pl.BlockSpec(memory_space=pltpu.VMEM)
ANY = pl.BlockSpec(memory_space=pl.ANY)
SMEM = pl.BlockSpec(memory_space=pltpu.SMEM)

H, C, PQ, PV, CZ = 12, 16, 4, 8, 128
HP = 16
WL = math.sqrt(1.0 / 3.0)
WC = math.sqrt(2.0 / (9.0 * PQ))
WS = 1.0 / math.sqrt(C)

F_PT = H * C
F_N1 = F_PT + 3 * H * PQ
F_N2 = F_N1 + HP
F_ALL = 384
G_PT = H * C
G_END = G_PT + 3 * H * PV
G_ALL = 512


def iota(shape, dim):
    return lax.broadcasted_iota(jnp.int32, shape, dim)


def head_of_feature(r):
    t = r - F_PT
    t = jnp.where(t >= 96, t - 96, jnp.where(t >= 48, t - 48, t))
    head = jnp.where(r < F_PT, r >> 4, t >> 2)
    head = jnp.where(r >= F_N1, r - F_N1, head)
    head = jnp.where(r >= F_N2, r - F_N2, head)
    return jnp.where(r >= F_N2 + HP, 99, head)


def head_of_value_feature(r):
    t = r - G_PT
    t = jnp.where(t >= 192, t - 192, jnp.where(t >= 96, t - 96, t))
    head = jnp.where(r < G_PT, r >> 4, t >> 3)
    return jnp.where(r >= G_END, 99, head)


def split2(x):
    hi = x.astype(BF16)
    return hi, (x - hi.astype(F32)).astype(BF16)


def split3(x):
    hi = x.astype(BF16)
    rest = x - hi.astype(F32)
    mid = rest.astype(BF16)
    return hi, mid, (rest - mid.astype(F32)).astype(BF16)


def mm(a, b):
    return jnp.dot(a, b, preferred_element_type=F32)


def mm_nt(a, b):
    return lax.dot_general(a, b, (((1,), (1,)), ((), ())), preferred_element_type=F32)


def softplus(x):
    return jnp.maximum(x, 0.0) + jnp.log(1.0 + jnp.exp(-jnp.abs(x)))


def coef_column(hw_ref, heads):
    coef = (0.5 * WL * WC) * softplus(hw_ref[...])
    rows = heads.shape[0]
    return jnp.sum(
        jnp.where(heads == iota((rows, H), 1), jnp.broadcast_to(coef, (rows, H)), 0.0),
        axis=1,
        keepdims=True,
    )


def rotate(rot, local, shift=None):
    out = []
    for x in range(3):
        t = rot[x][0] * local[0] + rot[x][1] * local[1] + rot[x][2] * local[2]
        out.append(t if shift is None else t + shift[x])
    return out


def pair_rows(head_rows, lane_block):
    keep = (iota(head_rows.shape, 0) >> 4) == lane_block
    return jnp.where(keep, head_rows, 0.0).astype(BF16)


def tile(k, size):
    return pl.ds(pl.multiple_of(k * size, size), size)


def mega(
    dims,
    pair_hbm,
    bw_ref,
    hw_ref,
    q_ref,
    k_ref,
    v_ref,
    qp_ref,
    kp_ref,
    vp_ref,
    rot_ref,
    tr_ref,
    count_ref,
    go_ref,
    gpt_ref,
    gpair_ref,
    ab_out,
    kfin_ref,
    qfin_ref,
    wfin_ref,
    pair_v,
    qf_s,
    kf_s,
    vf_s,
    gf_s,
    kt_s,
    kcat_s,
    qcat_s,
    vcat_s,
    gcat_s,
    kparts_s,
    vparts_s,
    w_s,
    g_s,
    p_s,
    pr_s,
    rhs_s,
    dh_s,
    dl_s,
    ah_s,
    al_s,
    kout_s,
    qout_s,
    st_s,
    xst_s,
    cst_s,
    zst_s,
    sc_s,
    kc_s,
    ksum_s,
    ky_s,
    kz_s,
    kr_s,
    qx_s,
    qz_s,
    qr_s,
    wm_s,
    wx_s,
    wz_s,
    wc_s,
    wy_s,
    wr_s,
    pair_sem,
    send_sem,
    recv_sem,
):
    nz, ny, nx, ni, nj = dims
    lanes = ni * HP
    groups = lanes // 128
    chunks = lanes // 256
    z, y, c = lax.axis_index("row_0"), lax.axis_index("row_1"), lax.axis_index("row_2")
    x, w = lax.axis_index("col_0"), lax.axis_index("col_1")

    for g in range(groups):
        pltpu.make_async_copy(
            pair_hbm.at[pl.ds(8 * g, 8)], pair_v.at[pl.ds(8 * g, 8)], pair_sem.at[g]
        ).start()

    barrier = pltpu.get_barrier_semaphore()
    peers = [{"row_2": 1 - c}, {"col_1": 1 - w}]
    peers += [{"row_1": lax.rem(y + r, ny)} for r in range(1, ny)]
    peers += [{"row_0": lax.rem(z + r, nz)} for r in range(1, nz)]
    peers += [{"col_0": lax.rem(x + r, nx)} for r in range(1, nx)]
    for peer in peers:
        pl.semaphore_signal(barrier, inc=1, device_id=peer, device_id_type=MESH)

    used = [0]

    def send(src, dst, peer):
        n = used[0]
        used[0] += 1
        copy = pltpu.make_async_remote_copy(
            src_ref=src,
            dst_ref=dst,
            send_sem=send_sem.at[n],
            recv_sem=recv_sem.at[n],
            device_id=peer,
            device_id_type=MESH,
        )
        copy.start()
        return copy

    base = pl.multiple_of((z * ny + y) * 128, 128)

    def own_half(full):
        return jnp.where(c == 1, pltpu.roll(full, 64, 1), full)[:, :ni]

    rot_q = []
    for a in range(3):
        t = own_half(rot_ref[a, :, pl.ds(base, 128)])
        rot_q.append([t[b : b + 1] for b in range(3)])
    t = own_half(tr_ref[:, pl.ds(base, 128)])
    tr_q = [t[a : a + 1] for a in range(3)]
    col = x * 2 + w
    kbase = tile(col, nj)
    rot_k = []
    for a in range(3):
        t = rot_ref[a, :, kbase]
        rot_k.append([t[b : b + 1] for b in range(3)])
    t = tr_ref[:, kbase]
    tr_k = [t[a : a + 1] for a in range(3)]

    norm_sel = ((iota((HP, 48), 1) >> 2) == iota((HP, 48), 0)).astype(F32)
    qg = rotate(rot_q, [qp_ref[b] for b in range(3)], tr_q)
    gg = rotate(rot_q, [gpt_ref[b] for b in range(3)])
    qf_s[0:F_PT] = q_ref[...]
    for a in range(3):
        qf_s[F_PT + 48 * a : F_PT + 48 * (a + 1)] = qg[a]
    qf_s[F_N1:F_N2] = jnp.ones((HP, ni), F32)
    qf_s[F_N2 : F_N2 + HP] = jnp.dot(
        norm_sel, qg[0] * qg[0] + qg[1] * qg[1] + qg[2] * qg[2], precision=HIGHEST
    )
    qf_s[F_N2 + HP :] = jnp.zeros((F_ALL - F_N2 - HP, ni), F32)
    gf_s[0:G_PT] = go_ref[...]
    for a in range(3):
        gf_s[G_PT + 96 * a : G_PT + 96 * (a + 1)] = gg[a]
    gf_s[G_END:] = jnp.zeros((G_ALL - G_END, ni), F32)

    kg = rotate(rot_k, [kp_ref[b] for b in range(3)], tr_k)
    vg = rotate(rot_k, [vp_ref[b] for b in range(3)], tr_k)
    kf_s[0:F_PT] = k_ref[...]
    for a in range(3):
        kf_s[F_PT + 48 * a : F_PT + 48 * (a + 1)] = kg[a]
    kf_s[F_N1:F_N2] = jnp.dot(
        norm_sel, kg[0] * kg[0] + kg[1] * kg[1] + kg[2] * kg[2], precision=HIGHEST
    )
    kf_s[F_N2 : F_N2 + HP] = jnp.ones((HP, nj), F32)
    kf_s[F_N2 + HP :] = jnp.zeros((F_ALL - F_N2 - HP, nj), F32)
    vf_s[0:G_PT] = v_ref[...]
    for a in range(3):
        vf_s[G_PT + 96 * a : G_PT + 96 * (a + 1)] = vg[a]
    vf_s[G_END:] = jnp.zeros((G_ALL - G_END, nj), F32)

    r = iota((F_ALL, 1), 0)
    coef = coef_column(hw_ref, head_of_feature(r))
    scale = jnp.where(r < F_PT, WL * WS, jnp.where(r < F_N1, 2.0 * coef, -coef))
    kt = jnp.transpose(kf_s[...] * scale)
    kt_s[...] = kt
    hi, mid, lo = split3(kt)
    for n, part in enumerate((hi, hi, mid, mid, hi, lo)):
        kcat_s[:, F_ALL * n : F_ALL * (n + 1)] = part
    hi, lo = split2(jnp.transpose(vf_s[...]))
    for n, part in enumerate((hi, hi, lo)):
        vcat_s[:, G_ALL * n : G_ALL * (n + 1)] = part
    kparts_s[0], kparts_s[1] = split2(kf_s[...])
    vparts_s[0], vparts_s[1] = split2(vf_s[G_PT:G_END])

    q_parts = split3(qf_s[...])
    g_parts = split2(gf_s[...])

    def expand(n, _):
        lane = iota((ni, 256), 1)
        e = ((lane >> 4) + n * 16 == iota((ni, 256), 0)).astype(BF16)
        for b in range(F_ALL // 128):
            head = head_of_feature(iota((128, 256), 0) + 128 * b)
            keep = head == (iota((128, 256), 1) & 15)
            hi, mid, lo = [
                jnp.where(keep, mm(part[128 * b : 128 * (b + 1)], e), 0.0).astype(BF16)
                for part in q_parts
            ]
            for m, part in enumerate((hi, mid, hi, mid, lo, hi)):
                at = F_ALL * m + 128 * b
                qcat_s[at : at + 128, tile(n, 256)] = part
        for b in range(G_ALL // 128):
            head = head_of_value_feature(iota((128, 256), 0) + 128 * b)
            keep = head == (iota((128, 256), 1) & 15)
            hi, lo = [
                jnp.where(keep, mm(part[128 * b : 128 * (b + 1)], e), 0.0).astype(BF16)
                for part in g_parts
            ]
            for m, part in enumerate((hi, lo, hi)):
                at = G_ALL * m + 128 * b
                gcat_s[at : at + 128, tile(n, 256)] = part
        return 0

    lax.fori_loop(0, chunks, expand, 0)

    w_s[...] = jnp.zeros((128, 128), F32)
    w_s[:, 0:H] = bw_ref[...].astype(F32)
    wt = jnp.transpose(w_s[...])[0:HP]
    g_s[...] = jnp.zeros((ni, HP, 128), F32)
    g_s[:, 0:H, :] = gpair_ref[...].astype(F32)
    w_rows = jnp.concatenate([wt] * 8, axis=0)
    for b in range(8):
        rhs_s[0:128, 128 * b : 128 * (b + 1)] = pair_rows(w_rows, b)

    count = count_ref[0]

    def forward(n, _):
        logits = mm(kcat_s[...], qcat_s[:, tile(n, 256)])
        prod = mm(vcat_s[...], gcat_s[:, tile(n, 256)])
        biases, prods = [], []
        for half in range(2):
            g = 2 * n + half
            pltpu.make_async_copy(
                pair_hbm.at[pl.ds(8 * g, 8)], pair_v.at[pl.ds(8 * g, 8)], pair_sem.at[g]
            ).wait()
            g_rows = g_s[pl.ds(8 * g, 8)].reshape(128, 128)
            for b in range(8):
                rhs_s[128:256, 128 * b : 128 * (b + 1)] = pair_rows(g_rows, b)
            acc = None
            for b in range(4):
                two = jnp.concatenate([pair_v[8 * g + 2 * b], pair_v[8 * g + 2 * b + 1]], axis=1)
                part = mm_nt(two, rhs_s[:, 256 * b : 256 * (b + 1)])
                acc = part if acc is None else acc + part
            biases.append(acc[:, :128])
            prods.append(acc[:, 128:])
        logits = logits + WL * jnp.concatenate(biases, axis=1)
        prod = prod + jnp.concatenate(prods, axis=1)
        valid = iota((nj, 256), 0) + col * nj < count
        logits = jnp.where(valid, logits, -1000000000.0)
        peak = jnp.max(logits, axis=0, keepdims=True)
        e = jnp.exp(logits - peak)
        p_s[:, tile(n, 256)] = e
        pr_s[:, tile(n, 256)] = prod
        total = jnp.sum(e, axis=0, keepdims=True)
        upper = jnp.sum(e * prod, axis=0, keepdims=True)
        for half in range(2):
            at = slice(128 * half, 128 * (half + 1))
            st_s[0, pl.ds(2 * n + half, 1), :] = peak[:, at]
            st_s[1, pl.ds(2 * n + half, 1), :] = total[:, at]
            st_s[2, pl.ds(2 * n + half, 1), :] = upper[:, at]
        return 0

    lax.fori_loop(0, chunks, forward, 0)

    pl.semaphore_wait(barrier, len(peers))
    copies = [send(st_s, xst_s.at[r - 1], {"col_0": lax.rem(x + r, nx)}) for r in range(1, nx)]
    for copy in copies:
        copy.wait()
    sets = [(st_s[0], st_s[1], st_s[2])]
    sets += [(xst_s[r, 0], xst_s[r, 1], xst_s[r, 2]) for r in range(nx - 1)]

    def merge(sets):
        peak = functools.reduce(jnp.maximum, [s[0] for s in sets])
        weights = [jnp.exp(s[0] - peak) for s in sets]
        total = sum(s[1] * f for s, f in zip(sets, weights))
        upper = sum(s[2] * f for s, f in zip(sets, weights))
        return peak, total, upper

    mine = merge(sets)
    for a in range(3):
        cst_s[a] = mine[a]
    send(cst_s, zst_s, {"col_1": 1 - w}).wait()
    peak, total, upper = merge([mine, (zst_s[0], zst_s[1], zst_s[2])])
    sc_s[0] = jnp.exp(st_s[0] - peak) / total
    sc_s[1] = upper / total

    def weights_of(g, acc):
        attn = p_s[:, tile(g, 128)] * sc_s[0, pl.ds(g, 1), :]
        dlog = attn * (pr_s[:, tile(g, 128)] - sc_s[1, pl.ds(g, 1), :])
        dh_s[:, tile(g, 128)], dl_s[:, tile(g, 128)] = split2(dlog)
        a_hi, a_lo = split2(attn)
        ah_s[:, tile(g, 128)] = a_hi
        al_s[:, tile(g, 128)] = a_lo
        scaled = WL * dlog
        ab_out[:, pl.ds(pl.multiple_of(g * 256, 256), 128)] = scaled.astype(BF16)
        ab_out[:, pl.ds(pl.multiple_of(g * 256 + 128, 128), 128)] = a_hi
        turned = jnp.transpose(scaled).astype(BF16)
        for b in range(8):
            acc = acc + mm(turned[16 * b : 16 * (b + 1)], pair_v[8 * g + b])
        return acc

    weight = lax.fori_loop(0, groups, weights_of, jnp.zeros((HP, 128), F32))

    kout = mm_nt(dh_s[...], qcat_s[0:F_ALL])
    kout += mm_nt(dh_s[...], qcat_s[F_ALL : 2 * F_ALL])
    kout += mm_nt(dl_s[...], qcat_s[0:F_ALL])
    aout = mm_nt(ah_s[...], gcat_s[0:G_ALL])
    aout += mm_nt(ah_s[...], gcat_s[G_ALL : 2 * G_ALL])
    aout += mm_nt(al_s[...], gcat_s[0:G_ALL])
    slab = nj // (nz * ny * 2)
    kout_s[:, :, :, 0:F_ALL] = kout.reshape(nz * ny, 2, slab, F_ALL)
    kout_s[:, :, :, F_ALL:] = aout.reshape(nz * ny, 2, slab, G_ALL)
    core_copy = send(kout_s.at[:, 1 - c], kc_s, {"row_2": 1 - c})
    spread = jnp.sum(kt_s[...] * kout, axis=0, keepdims=True)

    wm_s[0:H] = weight[0:H]
    wm_s[H : H + 1] = spread[:, 128:256]
    wm_s[H + 1 : H + 2] = spread[:, 256:384]
    wm_s[H + 2 :] = jnp.zeros((HP - H - 2, 128), F32)

    def share(src, slots, axis, me, count):
        slots[me] = src[...]
        return [send(src, slots.at[me], {axis: lax.rem(me + r, count)}) for r in range(1, count)]

    def settle(copies, slots, dst, count):
        for copy in copies:
            copy.wait()
        dst[...] = functools.reduce(lambda a, b: a + b, [slots[n] for n in range(count)])

    wx_copies = share(wm_s, wx_s, "col_0", x, nx)

    def query_side(n, acc):
        at = tile(n, 256)
        lane = iota((ni, 256), 1)
        e = ((lane >> 4) + n * 16 == iota((ni, 256), 0)).astype(BF16)
        outs = []
        for parts, hi_ref, lo_ref, head_of, rows, first in (
            (kparts_s, dh_s, dl_s, head_of_feature, F_ALL, 0),
            (vparts_s, ah_s, al_s, head_of_value_feature, G_END - G_PT, G_PT),
        ):
            full = mm(parts[0], hi_ref[:, at]) + mm(parts[0], lo_ref[:, at])
            full += mm(parts[1], hi_ref[:, at])
            keep = head_of(iota((rows, 256), 0) + first) == (iota((rows, 256), 1) & 15)
            hi, lo = split2(jnp.where(keep, full, 0.0))
            outs.append(mm_nt(e, hi) + mm_nt(e, lo))
        return acc[0] + outs[0], acc[1] + outs[1]

    q1, q2 = lax.fori_loop(
        0,
        chunks,
        query_side,
        (jnp.zeros((ni, F_ALL), F32), jnp.zeros((ni, G_END - G_PT), F32)),
    )
    qslab = ni // (nx * 2)
    qout_s[:, :, :, 0:F_ALL] = q1.reshape(nx, 2, qslab, F_ALL)
    qout_s[:, :, :, F_ALL : F_ALL + G_END - G_PT] = q2.reshape(nx, 2, qslab, G_END - G_PT)
    qout_s[:, :, :, F_ALL + G_END - G_PT :] = jnp.zeros(
        (nx, 2, qslab, qout_s.shape[3] - F_ALL - G_END + G_PT), F32
    )
    qx_copies = []
    for r in range(1, nx):
        peer = lax.rem(x + r, nx)
        qx_copies.append(send(qout_s.at[peer], qx_s.at[r - 1], {"col_0": peer}))

    core_copy.wait()
    ksum_s[...] = (kout_s[:, c] + kc_s[...]).reshape(ksum_s.shape)
    ky_copies = []
    for r in range(1, ny):
        peer = lax.rem(y + r, ny)
        ky_copies.append(send(ksum_s.at[:, peer], ky_s.at[r - 1], {"row_1": peer}))

    settle(wx_copies, wx_s, wm_s, nx)
    wz_copy = send(wm_s, wz_s, {"col_1": 1 - w})
    for copy in qx_copies:
        copy.wait()
    qz_s[...] = functools.reduce(lambda a, b: a + b, [qx_s[r] for r in range(nx - 1)], qout_s[x])
    qz_copy = send(qz_s.at[1 - w], qr_s, {"col_1": 1 - w})

    for copy in ky_copies:
        copy.wait()
    kz_s[...] = functools.reduce(lambda a, b: a + b, [ky_s[r] for r in range(ny - 1)], ksum_s[:, y])
    kz_copies = []
    for r in range(1, nz):
        peer = lax.rem(z + r, nz)
        kz_copies.append(send(kz_s.at[peer], kr_s.at[r - 1], {"row_0": peer}))

    wz_copy.wait()
    wm_s[...] = wm_s[...] + wz_s[...]
    wc_copy = send(wm_s, wc_s, {"row_2": 1 - c})
    wc_copy.wait()
    wm_s[...] = wm_s[...] + wc_s[...]
    wy_copies = share(wm_s, wy_s, "row_1", y, ny)
    qz_copy.wait()
    qfin_ref[...] = qz_s[w] + qr_s[...]
    settle(wy_copies, wy_s, wm_s, ny)
    wr_copies = share(wm_s, wr_s, "row_0", z, nz)
    for copy in kz_copies:
        copy.wait()
    kfin_ref[...] = functools.reduce(lambda a, b: a + b, [kr_s[r] for r in range(nz - 1)], kz_s[z])
    settle(wr_copies, wr_s, wfin_ref, nz)


def finish(
    dims,
    ab_ref,
    gpair_ref,
    bw_ref,
    hw_ref,
    kfin_ref,
    qfin_ref,
    wfin_ref,
    qp_ref,
    kp_ref,
    vp_ref,
    rot_ref,
    tr_ref,
    gpt_ref,
    pair_out,
    q_out,
    qp_out,
    qf_out,
    k_out,
    v_out,
    kp_out,
    vp_out,
    kf_out,
    w_out,
    hw_out,
    g_s,
    w_s,
    t_s,
    tq_s,
    rhs_s,
):
    nz, ny, nx, ni, nj = dims
    z, y, c = lax.axis_index("row_0"), lax.axis_index("row_1"), lax.axis_index("row_2")
    x, w = lax.axis_index("col_0"), lax.axis_index("col_1")
    row = (z * ny + y) * 2 + c
    col = x * 2 + w
    slab = nj // (nz * ny * 2)
    qslab = ni // (nx * 2)

    @pl.when(pl.program_id(0) == 0)
    def _():
        w_s[...] = jnp.zeros((128, 128), F32)
        w_s[:, 0:H] = bw_ref[...].astype(F32)
        w_rows = jnp.concatenate([jnp.transpose(w_s[...])[0:HP]] * 8, axis=0)
        for b in range(8):
            rhs_s[0:128, 128 * b : 128 * (b + 1)] = pair_rows(w_rows, b)
        g_s[...] = jnp.zeros(g_s.shape, F32)

    g_s[:, 0:H, :] = gpair_ref[...].astype(F32)
    g_rows = g_s[...].reshape(128, 128)
    for b in range(8):
        rhs_s[128:256, 128 * b : 128 * (b + 1)] = pair_rows(g_rows, b)
    for b in range(4):
        two = mm(ab_ref[...], rhs_s[:, 256 * b : 256 * (b + 1)]).astype(BF16)
        pair_out[2 * b] = two[:, :128]
        pair_out[2 * b + 1] = two[:, 128:]

    @pl.when(pl.program_id(0) == 0)
    def _():
        def pick(count, start):
            return (iota((count, 128), 0) == start + iota((count, 128), 1)).astype(F32)

        def exact(a, b):
            return jnp.dot(a, b, precision=HIGHEST)

        def split_rows(t):
            return [t[b : b + 1] for b in range(3)]

        expand = ((iota((48, HP), 0) >> 2) == iota((48, HP), 1)).astype(F32)
        coef = coef_column(hw_ref, iota((48, 1), 0) >> 2)

        at = row * slab
        sel = pick(128, lax.rem(at, 128))
        base = tile(col * (nj // 128) + at // 128, 128)
        here = tile(at // 128, 128)
        rot = [split_rows(exact(rot_ref[a, :, base], sel)) for a in range(3)]
        shift = split_rows(exact(tr_ref[:, base], sel))
        kp = [exact(kp_ref[b, :, here], sel) for b in range(3)]
        vp = [exact(vp_ref[b, :, here], sel) for b in range(3)]
        kg = rotate(rot, kp, shift)
        t_s[...] = jnp.zeros(t_s.shape, F32)
        t_s[0:slab] = kfin_ref[...]
        kt = jnp.transpose(t_s[...])
        k_out[...] = (WL * WS) * kt[0:F_PT, :slab]
        v_out[...] = kt[F_ALL : F_ALL + G_PT, :slab]
        sums = exact(expand, kt[F_N1:F_N2])
        dkg = [
            2.0 * coef * (kt[F_PT + 48 * a : F_PT + 48 * (a + 1)] - kg[a] * sums) for a in range(3)
        ]
        v_at = F_ALL + G_PT
        dvg = [kt[v_at + 96 * a : v_at + 96 * (a + 1)] for a in range(3)]
        for b in range(3):
            kp_out[b] = (rot[0][b] * dkg[0] + rot[1][b] * dkg[1] + rot[2][b] * dkg[2])[:, :slab]
            vp_out[b] = (rot[0][b] * dvg[0] + rot[1][b] * dvg[1] + rot[2][b] * dvg[2])[:, :slab]

        def over(t):
            return jnp.sum(t, axis=0, keepdims=True)

        for a in range(3):
            for b in range(3):
                kf_out[a, b : b + 1] = (over(dkg[a] * kp[b]) + over(dvg[a] * vp[b]))[:, :slab]
            kf_out[a, 3:4] = (over(dkg[a]) + over(dvg[a]))[:, :slab]

        inner = c * ni + col * qslab
        sel = pick(128, inner)
        base = tile(z * ny + y, 128)
        rot = [split_rows(exact(rot_ref[a, :, base], sel)) for a in range(3)]
        shift = split_rows(exact(tr_ref[:, base], sel))
        sel = pick(ni, col * qslab)
        qp = [exact(qp_ref[b], sel) for b in range(3)]
        gp = [exact(gpt_ref[b], sel) for b in range(3)]
        qg = rotate(rot, qp, shift)
        gg = rotate(rot, gp)
        tq_s[...] = jnp.zeros(tq_s.shape, F32)
        tq_s[0:qslab] = qfin_ref[...]
        qt = jnp.transpose(tq_s[...])
        q_out[...] = (WL * WS) * qt[0:F_PT, :qslab]
        sums = exact(expand, qt[F_N2 : F_N2 + HP])
        dqg = [
            -2.0 * coef * (qg[a] * sums - qt[F_PT + 48 * a : F_PT + 48 * (a + 1)]) for a in range(3)
        ]
        opt = [qt[F_ALL + 96 * a : F_ALL + 96 * (a + 1)] - shift[a] for a in range(3)]
        for b in range(3):
            qp_out[b] = (rot[0][b] * dqg[0] + rot[1][b] * dqg[1] + rot[2][b] * dqg[2])[:, :qslab]
        for a in range(3):
            for b in range(3):
                qf_out[a, b : b + 1] = (over(dqg[a] * qp[b]) + over(opt[a] * gp[b]))[:, :qslab]
            qf_out[a, 3:4] = (over(dqg[a]) - over(gg[a]))[:, :qslab]

        w_s[...] = jnp.zeros((128, 128), F32)
        w_s[0:HP] = wfin_ref[...]
        w_out[...] = jnp.transpose(w_s[...])[:, 0:H]
        total = jnp.zeros((1, 128), F32)
        for n in range(2):
            f = iota((128, 128), 0) + 128 * (n + 1)
            keep = (head_of_feature(f) == iota((128, 128), 1)) & (f >= F_PT)
            total += exact(wfin_ref[H + n : H + n + 1], keep.astype(F32))
        hw = hw_ref[...]
        hw_out[...] = total[:, 0:H] / (softplus(hw) * (1.0 + jnp.exp(-hw)))


def per_device(dims, *args):
    (pair, bw, hw, q, k, v, qp, kp, vp, rot, tr, count, go, gpt, gpair) = args
    nz, ny, nx, ni, nj = dims
    hw = hw.reshape(1, H)
    lanes = ni * HP
    slab, qslab = nj // (nz * ny * 2), ni // (nx * 2)
    kw, qw = F_ALL + G_ALL, 768
    groups = lanes // 128
    sends = 2 * ((nx - 1) + 1) + 1 + (ny - 1) + (nz - 1) + (nx - 1) + 1 + 1 + (ny - 1) + (nz - 1)

    def buf(*shape, dtype=F32):
        return pltpu.VMEM(shape, dtype)

    ab, kfin, qfin, wfin = pl.pallas_call(
        functools.partial(mega, dims),
        out_shape=[
            jax.ShapeDtypeStruct((nj, 2 * lanes), BF16),
            jax.ShapeDtypeStruct((slab, kw), F32),
            jax.ShapeDtypeStruct((qslab, qw), F32),
            jax.ShapeDtypeStruct((HP, 128), F32),
        ],
        in_specs=[ANY] + [VMEM] * 10 + [SMEM] + [VMEM] * 3,
        out_specs=[VMEM] * 4,
        scratch_shapes=[
            buf(ni, nj, CZ, dtype=BF16),
            buf(F_ALL, ni),
            buf(F_ALL, nj),
            buf(G_ALL, nj),
            buf(G_ALL, ni),
            buf(nj, F_ALL),
            buf(nj, 6 * F_ALL, dtype=BF16),
            buf(6 * F_ALL, lanes, dtype=BF16),
            buf(nj, 3 * G_ALL, dtype=BF16),
            buf(3 * G_ALL, lanes, dtype=BF16),
            buf(2, F_ALL, nj, dtype=BF16),
            buf(2, G_END - G_PT, nj, dtype=BF16),
            buf(128, 128),
            buf(ni, HP, 128),
            buf(nj, lanes),
            buf(nj, lanes),
            buf(256, 1024, dtype=BF16),
            buf(nj, lanes, dtype=BF16),
            buf(nj, lanes, dtype=BF16),
            buf(nj, lanes, dtype=BF16),
            buf(nj, lanes, dtype=BF16),
            buf(nz * ny, 2, slab, kw),
            buf(nx, 2, qslab, qw),
            buf(3, groups, 128),
            buf(nx - 1, 3, groups, 128),
            buf(3, groups, 128),
            buf(3, groups, 128),
            buf(2, groups, 128),
            buf(nz * ny, slab, kw),
            buf(nz, ny, slab, kw),
            buf(ny - 1, nz, slab, kw),
            buf(nz, slab, kw),
            buf(nz - 1, slab, kw),
            buf(nx - 1, 2, qslab, qw),
            buf(2, qslab, qw),
            buf(qslab, qw),
            buf(HP, 128),
            buf(nx, HP, 128),
            buf(HP, 128),
            buf(HP, 128),
            buf(ny, HP, 128),
            buf(nz, HP, 128),
            pltpu.SemaphoreType.DMA((groups,)),
            pltpu.SemaphoreType.DMA((sends,)),
            pltpu.SemaphoreType.DMA((sends,)),
        ],
        compiler_params=pltpu.CompilerParams(
            collective_id=0, has_side_effects=True, vmem_limit_bytes=56 * 2**20
        ),
        name="tile_and_reduce",
    )(pair, bw, hw, q, k, v, qp, kp, vp, rot, tr, count, go, gpt, gpair)

    def whole(a):
        return pl.BlockSpec(a.shape, lambda g, n=len(a.shape): (0,) * n)

    outs = [
        jax.ShapeDtypeStruct((ni, nj, CZ), BF16),
        jax.ShapeDtypeStruct((H * C, qslab), F32),
        jax.ShapeDtypeStruct((3, H * PQ, qslab), F32),
        jax.ShapeDtypeStruct((3, 4, qslab), F32),
        jax.ShapeDtypeStruct((H * C, slab), F32),
        jax.ShapeDtypeStruct((H * C, slab), F32),
        jax.ShapeDtypeStruct((3, H * PQ, slab), F32),
        jax.ShapeDtypeStruct((3, H * PV, slab), F32),
        jax.ShapeDtypeStruct((3, 4, slab), F32),
        jax.ShapeDtypeStruct((CZ, H), F32),
        jax.ShapeDtypeStruct((1, H), F32),
    ]
    small = [bw, hw, kfin, qfin, wfin, qp, kp, vp, rot, tr, gpt]
    res = pl.pallas_call(
        functools.partial(finish, dims),
        grid=(groups,),
        out_shape=outs,
        in_specs=[
            pl.BlockSpec((nj, 256), lambda g: (0, g)),
            pl.BlockSpec((8, H, CZ), lambda g: (g, 0, 0)),
        ]
        + [whole(a) for a in small],
        out_specs=[pl.BlockSpec((8, nj, CZ), lambda g: (g, 0, 0))] + [whole(a) for a in outs[1:]],
        scratch_shapes=[
            buf(8, HP, 128),
            buf(128, 128),
            buf(128, kw),
            buf(128, qw),
            buf(256, 1024, dtype=BF16),
        ],
        name="pair_and_frames",
    )(ab, gpair, *small)
    return (*res[:-1], res[-1].reshape(H))


def solution(mesh):
    finer = Mesh(mesh.devices.reshape(4, 4, 2, 4, 2), ("row_0", "row_1", "row_2", "col_0", "col_1"))
    return sharded(finer, 64, 256)


def sharded(finer, ni, nj):
    sizes = finer.shape
    dims = (sizes["row_0"], sizes["row_1"], sizes["col_0"], ni, nj)
    in_specs = (
        P(ROW, COL, None),
        P(),
        P(),
        P(None, ROW),
        P(None, COL),
        P(None, COL),
        P(None, None, ROW),
        P(None, None, COL),
        P(None, None, COL),
        P(),
        P(),
        P(),
        P(None, ROW),
        P(None, None, ROW),
        P(ROW, None, None),
    )
    out_specs = (
        P(ROW, COL, None),
        P(None, ROW_COL),
        P(None, None, ROW_COL),
        P(None, None, ROW_COL),
        P(None, COL_ROW),
        P(None, COL_ROW),
        P(None, None, COL_ROW),
        P(None, None, COL_ROW),
        P(None, None, COL_ROW),
        P(),
        P(),
    )
    return jax.shard_map(
        functools.partial(per_device, dims),
        mesh=finer,
        in_specs=in_specs,
        out_specs=out_specs,
        check_vma=False,
    )
```

```python
import functools
import math

import jax
import jax.numpy as jnp
from jax import lax
from jax.experimental import pallas as pl
from jax.experimental.pallas import tpu as pltpu
from jax.sharding import Mesh
from jax.sharding import PartitionSpec as P

ROW = ("row_0", "row_1", "row_2")
COL = ("col_0", "col_1")
ROW_COL = ("row_0", "row_1", "row_2", "col_0", "col_1")
COL_ROW = ("col_0", "col_1", "row_0", "row_1", "row_2")

MESH = pl.DeviceIdType.MESH
HIGHEST = lax.Precision.HIGHEST
F32 = jnp.float32
BF16 = jnp.bfloat16
VMEM = pl.BlockSpec(memory_space=pltpu.VMEM)
ANY = pl.BlockSpec(memory_space=pl.ANY)
SMEM = pl.BlockSpec(memory_space=pltpu.SMEM)

H, C, PQ, PV, CZ = 12, 16, 4, 8, 128
HP = 16
WL = math.sqrt(1.0 / 3.0)
WC = math.sqrt(2.0 / (9.0 * PQ))
WS = 1.0 / math.sqrt(C)

F_PT = H * C
F_N1 = F_PT + 3 * H * PQ
F_N2 = F_N1 + HP
F_ALL = 384
G_PT = H * C
G_END = G_PT + 3 * H * PV
G_ALL = 512


def iota(shape, dim):
    return lax.broadcasted_iota(jnp.int32, shape, dim)


def head_of_feature(r):
    t = r - F_PT
    t = jnp.where(t >= 96, t - 96, jnp.where(t >= 48, t - 48, t))
    head = jnp.where(r < F_PT, r >> 4, t >> 2)
    head = jnp.where(r >= F_N1, r - F_N1, head)
    head = jnp.where(r >= F_N2, r - F_N2, head)
    return jnp.where(r >= F_N2 + HP, 99, head)


def head_of_value_feature(r):
    t = r - G_PT
    t = jnp.where(t >= 192, t - 192, jnp.where(t >= 96, t - 96, t))
    head = jnp.where(r < G_PT, r >> 4, t >> 3)
    return jnp.where(r >= G_END, 99, head)


def split2(x):
    hi = x.astype(BF16)
    return hi, (x - hi.astype(F32)).astype(BF16)


def split3(x):
    hi = x.astype(BF16)
    rest = x - hi.astype(F32)
    mid = rest.astype(BF16)
    return hi, mid, (rest - mid.astype(F32)).astype(BF16)


def mm(a, b):
    return jnp.dot(a, b, preferred_element_type=F32)


def mm_nt(a, b):
    return lax.dot_general(a, b, (((1,), (1,)), ((), ())), preferred_element_type=F32)


def softplus(x):
    return jnp.maximum(x, 0.0) + jnp.log(1.0 + jnp.exp(-jnp.abs(x)))


def coef_column(hw_ref, heads):
    coef = (0.5 * WL * WC) * softplus(hw_ref[...])
    rows = heads.shape[0]
    return jnp.sum(
        jnp.where(heads == iota((rows, H), 1), jnp.broadcast_to(coef, (rows, H)), 0.0),
        axis=1,
        keepdims=True,
    )


def rotate(rot, local, shift=None):
    out = []
    for x in range(3):
        t = rot[x][0] * local[0] + rot[x][1] * local[1] + rot[x][2] * local[2]
        out.append(t if shift is None else t + shift[x])
    return out


def pair_rows(head_rows, lane_block):
    keep = (iota(head_rows.shape, 0) >> 4) == lane_block
    return jnp.where(keep, head_rows, 0.0).astype(BF16)


def tile(k, size):
    return pl.ds(pl.multiple_of(k * size, size), size)


def mega(
    dims,
    pair_hbm,
    bw_ref,
    hw_ref,
    q_ref,
    k_ref,
    v_ref,
    qp_ref,
    kp_ref,
    vp_ref,
    rot_ref,
    tr_ref,
    count_ref,
    go_ref,
    gpt_ref,
    gpair_ref,
    ab_out,
    kfin_ref,
    qfin_ref,
    wfin_ref,
    pair_v,
    qf_s,
    kf_s,
    vf_s,
    gf_s,
    kt_s,
    kcat_s,
    qcat_s,
    vcat_s,
    gcat_s,
    kparts_s,
    vparts_s,
    w_s,
    g_s,
    p_s,
    pr_s,
    rhs_s,
    dh_s,
    dl_s,
    ah_s,
    al_s,
    qout_s,
    st_s,
    xst_s,
    cst_s,
    zst_s,
    sc_s,
    s0_s,
    sc0_s,
    s1_s,
    sz_s,
    s2_s,
    sr_s,
    v0_s,
    vc0_s,
    v1_s,
    vy_s,
    v2_s,
    vr_s,
    qx_s,
    qz_s,
    qr_s,
    wm_s,
    wx_s,
    wz_s,
    wc_s,
    wy_s,
    wr_s,
    pair_sem,
    send_sem,
    recv_sem,
):
    nz, ny, nx, ni, nj = dims
    lanes = ni * HP
    groups = lanes // 128
    chunks = lanes // 256
    z, y, c = lax.axis_index("row_0"), lax.axis_index("row_1"), lax.axis_index("row_2")
    x, w = lax.axis_index("col_0"), lax.axis_index("col_1")

    for g in range(groups):
        pltpu.make_async_copy(
            pair_hbm.at[pl.ds(8 * g, 8)], pair_v.at[pl.ds(8 * g, 8)], pair_sem.at[g]
        ).start()

    barrier = pltpu.get_barrier_semaphore()
    peers = [{"row_2": 1 - c}, {"col_1": 1 - w}]
    peers += [{"row_1": lax.rem(y + r, ny)} for r in range(1, ny)]
    peers += [{"row_0": lax.rem(z + r, nz)} for r in range(1, nz)]
    peers += [{"col_0": lax.rem(x + r, nx)} for r in range(1, nx)]
    for peer in peers:
        pl.semaphore_signal(barrier, inc=1, device_id=peer, device_id_type=MESH)

    used = [0]

    def send(src, dst, peer):
        n = used[0]
        used[0] += 1
        copy = pltpu.make_async_remote_copy(
            src_ref=src,
            dst_ref=dst,
            send_sem=send_sem.at[n],
            recv_sem=recv_sem.at[n],
            device_id=peer,
            device_id_type=MESH,
        )
        copy.start()
        return copy

    base = pl.multiple_of((z * ny + y) * 128, 128)

    def own_half(full):
        return jnp.where(c == 1, pltpu.roll(full, 64, 1), full)[:, :ni]

    rot_q = []
    for a in range(3):
        t = own_half(rot_ref[a, :, pl.ds(base, 128)])
        rot_q.append([t[b : b + 1] for b in range(3)])
    t = own_half(tr_ref[:, pl.ds(base, 128)])
    tr_q = [t[a : a + 1] for a in range(3)]
    col = x * 2 + w
    kbase = tile(col, nj)
    rot_k = []
    for a in range(3):
        t = rot_ref[a, :, kbase]
        rot_k.append([t[b : b + 1] for b in range(3)])
    t = tr_ref[:, kbase]
    tr_k = [t[a : a + 1] for a in range(3)]

    norm_sel = ((iota((HP, 48), 1) >> 2) == iota((HP, 48), 0)).astype(F32)
    qg = rotate(rot_q, [qp_ref[b] for b in range(3)], tr_q)
    gg = rotate(rot_q, [jnp.transpose(gpt_ref[b]) for b in range(3)])
    qf_s[0:F_PT] = jnp.transpose(q_ref[...])
    for a in range(3):
        qf_s[F_PT + 48 * a : F_PT + 48 * (a + 1)] = qg[a]
    qf_s[F_N1:F_N2] = jnp.ones((HP, ni), F32)
    qf_s[F_N2 : F_N2 + HP] = jnp.dot(
        norm_sel, qg[0] * qg[0] + qg[1] * qg[1] + qg[2] * qg[2], precision=HIGHEST
    )
    qf_s[F_N2 + HP :] = jnp.zeros((F_ALL - F_N2 - HP, ni), F32)
    gf_s[0:G_PT] = jnp.transpose(go_ref[...])
    for a in range(3):
        gf_s[G_PT + 96 * a : G_PT + 96 * (a + 1)] = gg[a]
    gf_s[G_END:] = jnp.zeros((G_ALL - G_END, ni), F32)

    kg = rotate(rot_k, [kp_ref[b] for b in range(3)], tr_k)
    vg = rotate(rot_k, [vp_ref[b] for b in range(3)], tr_k)
    kf_s[0:F_PT] = k_ref[...]
    for a in range(3):
        kf_s[F_PT + 48 * a : F_PT + 48 * (a + 1)] = kg[a]
    kf_s[F_N1:F_N2] = jnp.dot(
        norm_sel, kg[0] * kg[0] + kg[1] * kg[1] + kg[2] * kg[2], precision=HIGHEST
    )
    kf_s[F_N2 : F_N2 + HP] = jnp.ones((HP, nj), F32)
    kf_s[F_N2 + HP :] = jnp.zeros((F_ALL - F_N2 - HP, nj), F32)
    vf_s[0:G_PT] = v_ref[...]
    for a in range(3):
        vf_s[G_PT + 96 * a : G_PT + 96 * (a + 1)] = vg[a]
    vf_s[G_END:] = jnp.zeros((G_ALL - G_END, nj), F32)

    r = iota((F_ALL, 1), 0)
    coef = coef_column(hw_ref, head_of_feature(r))
    scale = jnp.where(r < F_PT, WL * WS, jnp.where(r < F_N1, 2.0 * coef, -coef))
    kt = jnp.transpose(kf_s[...] * scale)
    kt_s[...] = kt
    hi, mid, lo = split3(kt)
    for n, part in enumerate((hi, hi, mid, mid, hi, lo)):
        kcat_s[:, F_ALL * n : F_ALL * (n + 1)] = part
    hi, lo = split2(jnp.transpose(vf_s[...]))
    for n, part in enumerate((hi, hi, lo)):
        vcat_s[:, G_ALL * n : G_ALL * (n + 1)] = part
    kparts_s[0], kparts_s[1] = split2(kf_s[...])
    vparts_s[0], vparts_s[1] = split2(vf_s[G_PT:G_END])

    q_parts = split3(qf_s[...])
    g_parts = split2(gf_s[...])

    def expand(n, _):
        lane = iota((ni, 256), 1)
        e = ((lane >> 4) + n * 16 == iota((ni, 256), 0)).astype(BF16)
        for b in range(F_ALL // 128):
            head = head_of_feature(iota((128, 256), 0) + 128 * b)
            keep = head == (iota((128, 256), 1) & 15)
            hi, mid, lo = [
                jnp.where(keep, mm(part[128 * b : 128 * (b + 1)], e), 0.0).astype(BF16)
                for part in q_parts
            ]
            for m, part in enumerate((hi, mid, hi, mid, lo, hi)):
                at = F_ALL * m + 128 * b
                qcat_s[at : at + 128, tile(n, 256)] = part
        for b in range(G_ALL // 128):
            head = head_of_value_feature(iota((128, 256), 0) + 128 * b)
            keep = head == (iota((128, 256), 1) & 15)
            hi, lo = [
                jnp.where(keep, mm(part[128 * b : 128 * (b + 1)], e), 0.0).astype(BF16)
                for part in g_parts
            ]
            for m, part in enumerate((hi, lo, hi)):
                at = G_ALL * m + 128 * b
                gcat_s[at : at + 128, tile(n, 256)] = part
        return 0

    lax.fori_loop(0, chunks, expand, 0)

    w_s[...] = jnp.zeros((HP, 128), F32)
    w_s[0:H] = bw_ref[...].astype(F32)
    g_s[...] = jnp.zeros((lanes, 128), F32)
    for b in range(H):
        g_s[pl.ds(b, ni, stride=HP), :] = gpair_ref[b].astype(F32)
    w_rows = jnp.concatenate([w_s[...]] * 8, axis=0)
    for b in range(8):
        rhs_s[0:128, 128 * b : 128 * (b + 1)] = pair_rows(w_rows, b)

    count = count_ref[0]

    def forward(n, _):
        logits = mm(kcat_s[...], qcat_s[:, tile(n, 256)])
        prod = mm(vcat_s[...], gcat_s[:, tile(n, 256)])
        biases, prods = [], []
        for half in range(2):
            g = 2 * n + half
            pltpu.make_async_copy(
                pair_hbm.at[pl.ds(8 * g, 8)], pair_v.at[pl.ds(8 * g, 8)], pair_sem.at[g]
            ).wait()
            g_rows = g_s[tile(g, 128)]
            for b in range(8):
                rhs_s[128:256, 128 * b : 128 * (b + 1)] = pair_rows(g_rows, b)
            acc = None
            for b in range(4):
                two = jnp.concatenate([pair_v[8 * g + 2 * b], pair_v[8 * g + 2 * b + 1]], axis=1)
                part = mm_nt(two, rhs_s[:, 256 * b : 256 * (b + 1)])
                acc = part if acc is None else acc + part
            biases.append(acc[:, :128])
            prods.append(acc[:, 128:])
        logits = logits + WL * jnp.concatenate(biases, axis=1)
        prod = prod + jnp.concatenate(prods, axis=1)
        valid = iota((nj, 256), 0) + col * nj < count
        logits = jnp.where(valid, logits, -1000000000.0)
        peak = jnp.max(logits, axis=0, keepdims=True)
        e = jnp.exp(logits - peak)
        p_s[:, tile(n, 256)] = e
        pr_s[:, tile(n, 256)] = prod
        total = jnp.sum(e, axis=0, keepdims=True)
        upper = jnp.sum(e * prod, axis=0, keepdims=True)
        for half in range(2):
            at = slice(128 * half, 128 * (half + 1))
            st_s[0, pl.ds(2 * n + half, 1), :] = peak[:, at]
            st_s[1, pl.ds(2 * n + half, 1), :] = total[:, at]
            st_s[2, pl.ds(2 * n + half, 1), :] = upper[:, at]
        return 0

    lax.fori_loop(0, chunks, forward, 0)

    pl.semaphore_wait(barrier, len(peers))
    copies = [send(st_s, xst_s.at[r - 1], {"col_0": lax.rem(x + r, nx)}) for r in range(1, nx)]
    for copy in copies:
        copy.wait()
    sets = [(st_s[0], st_s[1], st_s[2])]
    sets += [(xst_s[r, 0], xst_s[r, 1], xst_s[r, 2]) for r in range(nx - 1)]

    def merge(sets):
        peak = functools.reduce(jnp.maximum, [s[0] for s in sets])
        weights = [jnp.exp(s[0] - peak) for s in sets]
        total = sum(s[1] * f for s, f in zip(sets, weights))
        upper = sum(s[2] * f for s, f in zip(sets, weights))
        return peak, total, upper

    mine = merge(sets)
    for a in range(3):
        cst_s[a] = mine[a]
    send(cst_s, zst_s, {"col_1": 1 - w}).wait()
    peak, total, upper = merge([mine, (zst_s[0], zst_s[1], zst_s[2])])
    sc_s[0] = jnp.exp(st_s[0] - peak) / total
    sc_s[1] = upper / total

    def weights_of(g, acc):
        attn = p_s[:, tile(g, 128)] * sc_s[0, pl.ds(g, 1), :]
        dlog = attn * (pr_s[:, tile(g, 128)] - sc_s[1, pl.ds(g, 1), :])
        dh_s[:, tile(g, 128)], dl_s[:, tile(g, 128)] = split2(dlog)
        a_hi, a_lo = split2(attn)
        ah_s[:, tile(g, 128)] = a_hi
        al_s[:, tile(g, 128)] = a_lo
        scaled = WL * dlog
        ab_out[:, pl.ds(pl.multiple_of(g * 256, 256), 128)] = scaled.astype(BF16)
        ab_out[:, pl.ds(pl.multiple_of(g * 256 + 128, 128), 128)] = a_hi
        turned = jnp.transpose(dlog).astype(BF16)
        for b in range(8):
            acc = acc + mm(turned[16 * b : 16 * (b + 1)], pair_v[8 * g + b])
        return acc

    weight = lax.fori_loop(0, groups, weights_of, jnp.zeros((HP, 128), F32))

    slab = nj // (nz * ny * 2)

    def add(terms):
        return functools.reduce(lambda a, b: a + b, terms)

    def spread_to(src, dst, axis, me, count, slot):
        out = []
        for r in range(1, count):
            peer = lax.rem(me + r, count)
            out.append(send(src.at[slot(peer)], dst.at[r - 1], {axis: peer}))
        return out

    def done(copies):
        for copy in copies:
            copy.wait()

    kout = mm_nt(dh_s[...], qcat_s[0:F_ALL])
    kout += mm_nt(dh_s[...], qcat_s[F_ALL : 2 * F_ALL])
    kout += mm_nt(dl_s[...], qcat_s[0:F_ALL])
    s0_s[...] = kout.reshape(s0_s.shape)
    s_core = send(s0_s.at[:, :, 1 - c], sc0_s, {"row_2": 1 - c})
    spread = jnp.sum(kt_s[...] * kout, axis=0, keepdims=True)

    wm_s[0:H] = WL * weight[0:H]
    wm_s[H : H + 1] = spread[:, 128:256]
    wm_s[H + 1 : H + 2] = spread[:, 256:384]
    wm_s[H + 2 :] = jnp.zeros((HP - H - 2, 128), F32)

    def share(src, slots, axis, me, count):
        slots[me] = src[...]
        return [send(src, slots.at[me], {axis: lax.rem(me + r, count)}) for r in range(1, count)]

    def settle(copies, slots, dst, count):
        done(copies)
        dst[...] = add([slots[n] for n in range(count)])

    w_x = share(wm_s, wx_s, "col_0", x, nx)

    aout = mm_nt(ah_s[...], gcat_s[0:G_ALL])
    aout += mm_nt(ah_s[...], gcat_s[G_ALL : 2 * G_ALL])
    aout += mm_nt(al_s[...], gcat_s[0:G_ALL])
    v0_s[...] = aout.reshape(v0_s.shape)
    v_core = send(v0_s.at[:, :, 1 - c], vc0_s, {"row_2": 1 - c})

    s_core.wait()
    s1_s[...] = s0_s[:, :, c] + sc0_s[...]
    s_z = spread_to(s1_s, sz_s, "row_0", z, nz, lambda p: p)
    v_core.wait()
    v1_s[...] = v0_s[:, :, c] + vc0_s[...]
    v_y = spread_to(v1_s, vy_s, "row_1", y, ny, lambda p: (slice(None), p))

    def query_side(n, acc):
        at = tile(n, 256)
        lane = iota((ni, 256), 1)
        e = ((lane >> 4) + n * 16 == iota((ni, 256), 0)).astype(BF16)
        outs = []
        for parts, hi_ref, lo_ref, head_of, rows, first in (
            (kparts_s, dh_s, dl_s, head_of_feature, F_ALL, 0),
            (vparts_s, ah_s, al_s, head_of_value_feature, G_END - G_PT, G_PT),
        ):
            full = mm(parts[0], hi_ref[:, at]) + mm(parts[0], lo_ref[:, at])
            full += mm(parts[1], hi_ref[:, at])
            keep = head_of(iota((rows, 256), 0) + first) == (iota((rows, 256), 1) & 15)
            hi, lo = split2(jnp.where(keep, full, 0.0))
            outs.append(mm_nt(e, hi) + mm_nt(e, lo))
        return acc[0] + outs[0], acc[1] + outs[1]

    sums = (jnp.zeros((ni, F_ALL), F32), jnp.zeros((ni, G_END - G_PT), F32))
    sums = lax.fori_loop(0, chunks // 2, query_side, sums)
    settle(w_x, wx_s, wm_s, nx)
    w_w = send(wm_s, wz_s, {"col_1": 1 - w})
    q1, q2 = lax.fori_loop(chunks // 2, chunks, query_side, sums)
    qslab = ni // (nx * 2)
    qout_s[:, :, :, 0:F_ALL] = q1.reshape(nx, 2, qslab, F_ALL)
    qout_s[:, :, :, F_ALL : F_ALL + G_END - G_PT] = q2.reshape(nx, 2, qslab, G_END - G_PT)
    qout_s[:, :, :, F_ALL + G_END - G_PT :] = jnp.zeros(
        (nx, 2, qslab, qout_s.shape[3] - F_ALL - G_END + G_PT), F32
    )
    q_x = spread_to(qout_s, qx_s, "col_0", x, nx, lambda p: p)

    done(s_z)
    s2_s[...] = add([s1_s[z]] + [sz_s[r] for r in range(nz - 1)])
    s_y = spread_to(s2_s, sr_s, "row_1", y, ny, lambda p: p)
    w_w.wait()
    wm_s[...] = wm_s[...] + wz_s[...]
    w_c = send(wm_s, wc_s, {"row_2": 1 - c})
    done(v_y)
    v2_s[...] = add([v1_s[:, y]] + [vy_s[r] for r in range(ny - 1)])
    v_z = spread_to(v2_s, vr_s, "row_0", z, nz, lambda p: p)
    w_c.wait()
    wm_s[...] = wm_s[...] + wc_s[...]
    w_y = share(wm_s, wy_s, "row_1", y, ny)
    done(q_x)
    qz_s[...] = add([qout_s[x]] + [qx_s[r] for r in range(nx - 1)])
    q_w = send(qz_s.at[1 - w], qr_s, {"col_1": 1 - w})
    settle(w_y, wy_s, wm_s, ny)
    w_z = share(wm_s, wr_s, "row_0", z, nz)
    done(s_y)
    kfin_ref[:, 0:F_ALL] = add([s2_s[y]] + [sr_s[r] for r in range(ny - 1)])
    done(v_z)
    kfin_ref[:, F_ALL:] = add([v2_s[z]] + [vr_s[r] for r in range(nz - 1)])
    q_w.wait()
    qfin_ref[...] = qz_s[w] + qr_s[...]
    settle(w_z, wr_s, wfin_ref, nz)


def finish(
    dims,
    ab_ref,
    gpair_ref,
    bw_ref,
    hw_ref,
    kfin_ref,
    qfin_ref,
    wfin_ref,
    qp_ref,
    kp_ref,
    vp_ref,
    rot_ref,
    tr_ref,
    gpt_ref,
    pair_out,
    q_out,
    qp_out,
    qf_out,
    k_out,
    v_out,
    kp_out,
    vp_out,
    kf_out,
    w_out,
    hw_out,
    g_s,
    w_s,
    t_s,
    rhs_s,
    pair_v,
    pair_sem,
):
    nz, ny, nx, ni, nj = dims
    z, y, c = lax.axis_index("row_0"), lax.axis_index("row_1"), lax.axis_index("row_2")
    x, w = lax.axis_index("col_0"), lax.axis_index("col_1")
    row = (z * ny + y) * 2 + c
    col = x * 2 + w
    slab = nj // (nz * ny * 2)
    qslab = ni // (nx * 2)

    w_s[...] = jnp.zeros((HP, 128), F32)
    w_s[0:H] = bw_ref[...].astype(F32)
    w_rows = jnp.concatenate([w_s[...]] * 8, axis=0)
    for b in range(8):
        rhs_s[0:128, 128 * b : 128 * (b + 1)] = pair_rows(w_rows, b)
    g_s[...] = jnp.zeros(g_s.shape, F32)
    for b in range(H):
        g_s[pl.ds(b, ni, stride=HP), :] = gpair_ref[b].astype(F32)

    def copy_out(g):
        at = pl.ds(pl.multiple_of(8 * g, 8), 8)
        return pltpu.make_async_copy(pair_v.at[at], pair_out.at[at], pair_sem.at[g])

    groups = ni // 8

    def pair_group(g, _):
        g_rows = g_s[tile(g, 128)]
        for b in range(8):
            rhs_s[128:256, 128 * b : 128 * (b + 1)] = pair_rows(g_rows, b)
        for b in range(4):
            two = mm(ab_ref[:, tile(g, 256)], rhs_s[:, 256 * b : 256 * (b + 1)]).astype(BF16)
            pair_v[8 * g + 2 * b] = two[:, :128]
            pair_v[8 * g + 2 * b + 1] = two[:, 128:]
        copy_out(g).start()
        return 0

    lax.fori_loop(0, groups, pair_group, 0)

    def exact(a, b):
        return jnp.dot(a, b, precision=HIGHEST)

    def from_lane(rows, at):
        return pltpu.roll(rows, lax.rem(128 - at, 128), 1)

    def over(t):
        return jnp.sum(t, axis=1, keepdims=True)

    def columns(t):
        return [[t[:, 3 * a + b : 3 * a + b + 1] for b in range(3)] for a in range(3)]

    def back(rot, v):
        return [rot[0][b] * v[0] + rot[1][b] * v[1] + rot[2][b] * v[2] for b in range(3)]

    def frame(out, cols, count):
        t = jnp.zeros((count, 128), F32)
        for n in range(12):
            t = jnp.where(iota((count, 128), 1) == n, cols[n // 4][n % 4], t)
        t_s[0:count] = t
        turned = jnp.transpose(t_s[0:128])
        for a in range(3):
            out[a] = turned[4 * a : 4 * a + 4, :count]

    expand = (iota((HP, 48), 0) == (iota((HP, 48), 1) >> 2)).astype(F32)
    coef = jnp.broadcast_to(coef_column(hw_ref, iota((48, 1), 0) >> 2), (48, 48))
    coef = jnp.where(iota((48, 48), 0) == iota((48, 48), 1), coef, 0.0)
    coef = jnp.sum(coef, axis=0, keepdims=True)

    t_s[...] = jnp.zeros(t_s.shape, F32)
    at = row * slab
    base = tile(col * (nj // 128) + at // 128, 128)
    here = tile(at // 128, 128)
    for a in range(3):
        t_s[3 * a : 3 * a + 3] = rot_ref[a, :, base]
        t_s[16 + 48 * a : 16 + 48 * (a + 1)] = kp_ref[a, :, here]
        t_s[160 + 96 * a : 160 + 96 * (a + 1)] = vp_ref[a, :, here]
    t_s[9:12] = tr_ref[:, base]
    own = jnp.transpose(from_lane(t_s[...], lax.rem(at, 128)))[:slab]
    rot = columns(own)
    shift = [own[:, 9 + a : 10 + a] for a in range(3)]
    kp = [own[:, 16 + 48 * b : 16 + 48 * (b + 1)] for b in range(3)]
    vp = [own[:, 160 + 96 * b : 160 + 96 * (b + 1)] for b in range(3)]
    kg = rotate(rot, kp, shift)
    k_out[...] = (WL * WS) * kfin_ref[:, 0:F_PT]
    v_out[...] = kfin_ref[:, F_ALL : F_ALL + G_PT]
    sums = exact(kfin_ref[:, F_N1:F_N2], expand)
    dkg = []
    for a in range(3):
        part = kfin_ref[:, F_PT + 48 * a : F_PT + 48 * (a + 1)]
        dkg.append(2.0 * coef * (part - kg[a] * sums))
    v_at = F_ALL + G_PT
    dvg = [kfin_ref[:, v_at + 96 * a : v_at + 96 * (a + 1)] for a in range(3)]
    for b, (dk, dv) in enumerate(zip(back(rot, dkg), back(rot, dvg))):
        kp_out[b] = dk
        vp_out[b] = dv
    cols = []
    for a in range(3):
        cols.append([over(dkg[a] * kp[b]) + over(dvg[a] * vp[b]) for b in range(3)])
        cols[a].append(over(dkg[a]) + over(dvg[a]))
    frame(kf_out, cols, slab)

    at = col * qslab
    base = tile(z * ny + y, 128)
    t_s[...] = jnp.zeros(t_s.shape, F32)
    for a in range(3):
        t_s[3 * a : 3 * a + 3] = rot_ref[a, :, base]
        t_s[16 + 48 * a : 16 + 48 * (a + 1), 0:ni] = qp_ref[a]
    t_s[9:12] = tr_ref[:, base]
    t_s[0:16] = from_lane(t_s[0:16], c * ni + at)
    t_s[16:160] = from_lane(t_s[16:160], at)
    own = jnp.transpose(t_s[0:256])[:qslab]
    rot = columns(own)
    shift = [own[:, 9 + a : 10 + a] for a in range(3)]
    qp = [own[:, 16 + 48 * b : 16 + 48 * (b + 1)] for b in range(3)]
    gp = [gpt_ref[b, tile(col, qslab), :] for b in range(3)]
    qg = rotate(rot, qp, shift)
    gg = rotate(rot, gp)
    q_out[...] = (WL * WS) * qfin_ref[:, 0:F_PT]
    sums = exact(qfin_ref[:, F_N2 : F_N2 + HP], expand)
    dqg = []
    for a in range(3):
        part = qfin_ref[:, F_PT + 48 * a : F_PT + 48 * (a + 1)]
        dqg.append(-2.0 * coef * (qg[a] * sums - part))
    opt = [qfin_ref[:, F_ALL + 96 * a : F_ALL + 96 * (a + 1)] - shift[a] for a in range(3)]
    for b, dq in enumerate(back(rot, dqg)):
        qp_out[b] = dq
    cols = []
    for a in range(3):
        cols.append([over(dqg[a] * qp[b]) + over(opt[a] * gp[b]) for b in range(3)])
        cols[a].append(over(dqg[a]) - over(gg[a]))
    frame(qf_out, cols, qslab)

    w_out[...] = wfin_ref[0:H]
    total = jnp.zeros((1, 128), F32)
    for n in range(2):
        f = iota((128, 128), 0) + 128 * (n + 1)
        keep = (head_of_feature(f) == iota((128, 128), 1)) & (f >= F_PT)
        total += exact(wfin_ref[H + n : H + n + 1], keep.astype(F32))
    hw = hw_ref[...]
    hw_out[...] = total[:, 0:H] / (softplus(hw) * (1.0 + jnp.exp(-hw)))

    for g in range(groups):
        copy_out(g).wait()


def per_device(dims, *args):
    (pair, bw, hw, q, k, v, qp, kp, vp, rot, tr, count, go, gpt, gpair) = args
    nz, ny, nx, ni, nj = dims
    hw = hw.reshape(1, H)
    bw, q, go = bw.T, q.T, go.T
    gpt = jnp.transpose(gpt, (0, 2, 1))
    gpair = jnp.transpose(gpair, (1, 0, 2))
    lanes = ni * HP
    slab, qslab = nj // (nz * ny * 2), ni // (nx * 2)
    kw, qw = F_ALL + G_ALL, 768
    groups = lanes // 128
    sends = 3 * nx + 3 * (ny - 1) + 3 * (nz - 1) + 3

    def buf(*shape, dtype=F32):
        return pltpu.VMEM(shape, dtype)

    ab, kfin, qfin, wfin = pl.pallas_call(
        functools.partial(mega, dims),
        out_shape=[
            jax.ShapeDtypeStruct((nj, 2 * lanes), BF16),
            jax.ShapeDtypeStruct((slab, kw), F32),
            jax.ShapeDtypeStruct((qslab, qw), F32),
            jax.ShapeDtypeStruct((HP, 128), F32),
        ],
        in_specs=[ANY] + [VMEM] * 10 + [SMEM] + [VMEM] * 3,
        out_specs=[VMEM] * 4,
        scratch_shapes=[
            buf(ni, nj, CZ, dtype=BF16),
            buf(F_ALL, ni),
            buf(F_ALL, nj),
            buf(G_ALL, nj),
            buf(G_ALL, ni),
            buf(nj, F_ALL),
            buf(nj, 6 * F_ALL, dtype=BF16),
            buf(6 * F_ALL, lanes, dtype=BF16),
            buf(nj, 3 * G_ALL, dtype=BF16),
            buf(3 * G_ALL, lanes, dtype=BF16),
            buf(2, F_ALL, nj, dtype=BF16),
            buf(2, G_END - G_PT, nj, dtype=BF16),
            buf(HP, 128),
            buf(lanes, 128),
            buf(nj, lanes),
            buf(nj, lanes),
            buf(256, 1024, dtype=BF16),
            buf(nj, lanes, dtype=BF16),
            buf(nj, lanes, dtype=BF16),
            buf(nj, lanes, dtype=BF16),
            buf(nj, lanes, dtype=BF16),
            buf(nx, 2, qslab, qw),
            buf(3, groups, 128),
            buf(nx - 1, 3, groups, 128),
            buf(3, groups, 128),
            buf(3, groups, 128),
            buf(2, groups, 128),
            buf(nz, ny, 2, slab, F_ALL),
            buf(nz, ny, slab, F_ALL),
            buf(nz, ny, slab, F_ALL),
            buf(nz - 1, ny, slab, F_ALL),
            buf(ny, slab, F_ALL),
            buf(ny - 1, slab, F_ALL),
            buf(nz, ny, 2, slab, G_ALL),
            buf(nz, ny, slab, G_ALL),
            buf(nz, ny, slab, G_ALL),
            buf(ny - 1, nz, slab, G_ALL),
            buf(nz, slab, G_ALL),
            buf(nz - 1, slab, G_ALL),
            buf(nx - 1, 2, qslab, qw),
            buf(2, qslab, qw),
            buf(qslab, qw),
            buf(HP, 128),
            buf(nx, HP, 128),
            buf(HP, 128),
            buf(HP, 128),
            buf(ny, HP, 128),
            buf(nz, HP, 128),
            pltpu.SemaphoreType.DMA((groups,)),
            pltpu.SemaphoreType.DMA((sends,)),
            pltpu.SemaphoreType.DMA((sends,)),
        ],
        compiler_params=pltpu.CompilerParams(
            collective_id=0, has_side_effects=True, vmem_limit_bytes=60 * 2**20
        ),
        name="tile_and_reduce",
    )(pair, bw, hw, q, k, v, qp, kp, vp, rot, tr, count, go, gpt, gpair)

    outs = [
        jax.ShapeDtypeStruct((ni, nj, CZ), BF16),
        jax.ShapeDtypeStruct((qslab, H * C), F32),
        jax.ShapeDtypeStruct((3, qslab, H * PQ), F32),
        jax.ShapeDtypeStruct((3, 4, qslab), F32),
        jax.ShapeDtypeStruct((slab, H * C), F32),
        jax.ShapeDtypeStruct((slab, H * C), F32),
        jax.ShapeDtypeStruct((3, slab, H * PQ), F32),
        jax.ShapeDtypeStruct((3, slab, H * PV), F32),
        jax.ShapeDtypeStruct((3, 4, slab), F32),
        jax.ShapeDtypeStruct((H, CZ), F32),
        jax.ShapeDtypeStruct((1, H), F32),
    ]
    small = [bw, hw, kfin, qfin, wfin, qp, kp, vp, rot, tr, gpt]
    res = pl.pallas_call(
        functools.partial(finish, dims),
        out_shape=outs,
        in_specs=[VMEM] * 13,
        out_specs=[ANY] + [VMEM] * 10,
        scratch_shapes=[
            buf(lanes, 128),
            buf(HP, 128),
            buf(512, 128),
            buf(256, 1024, dtype=BF16),
            buf(ni, nj, CZ, dtype=BF16),
            pltpu.SemaphoreType.DMA((groups,)),
        ],
        compiler_params=pltpu.CompilerParams(vmem_limit_bytes=60 * 2**20),
        name="pair_and_frames",
    )(ab, gpair, *small)
    pair_grad, dq, dqp, dqf, dk, dv, dkp, dvp, dkf, dw, dhw = res
    turn = functools.partial(jnp.transpose, axes=(0, 2, 1))
    return pair_grad, dq.T, turn(dqp), dqf, dk.T, dv.T, turn(dkp), turn(dvp), dkf, dw.T, dhw[0]


def solution(mesh):
    finer = Mesh(mesh.devices.reshape(4, 4, 2, 4, 2), ("row_0", "row_1", "row_2", "col_0", "col_1"))
    return sharded(finer, 64, 256)


def sharded(finer, ni, nj):
    sizes = finer.shape
    dims = (sizes["row_0"], sizes["row_1"], sizes["col_0"], ni, nj)
    in_specs = (
        P(ROW, COL, None),
        P(),
        P(),
        P(None, ROW),
        P(None, COL),
        P(None, COL),
        P(None, None, ROW),
        P(None, None, COL),
        P(None, None, COL),
        P(),
        P(),
        P(),
        P(None, ROW),
        P(None, None, ROW),
        P(ROW, None, None),
    )
    out_specs = (
        P(ROW, COL, None),
        P(None, ROW_COL),
        P(None, None, ROW_COL),
        P(None, None, ROW_COL),
        P(None, COL_ROW),
        P(None, COL_ROW),
        P(None, None, COL_ROW),
        P(None, None, COL_ROW),
        P(None, None, COL_ROW),
        P(),
        P(),
    )
    return jax.shard_map(
        functools.partial(per_device, dims),
        mesh=finer,
        in_specs=in_specs,
        out_specs=out_specs,
        check_vma=False,
    )
```

```python
import functools
import math

import jax
import jax.numpy as jnp
from jax import lax
from jax.experimental import pallas as pl
from jax.experimental.pallas import tpu as pltpu
from jax.sharding import Mesh
from jax.sharding import PartitionSpec as P

ROW = ("row_0", "row_1", "row_2")
COL = ("col_0", "col_1")
ROW_COL = ("row_0", "row_1", "row_2", "col_0", "col_1")
COL_ROW = ("col_0", "col_1", "row_0", "row_1", "row_2")

MESH = pl.DeviceIdType.MESH
HIGHEST = lax.Precision.HIGHEST
F32 = jnp.float32
BF16 = jnp.bfloat16
VMEM = pl.BlockSpec(memory_space=pltpu.VMEM)
ANY = pl.BlockSpec(memory_space=pl.ANY)
SMEM = pl.BlockSpec(memory_space=pltpu.SMEM)

H, C, PQ, PV, CZ = 12, 16, 4, 8, 128
HP = 16
WL = math.sqrt(1.0 / 3.0)
WC = math.sqrt(2.0 / (9.0 * PQ))
WS = 1.0 / math.sqrt(C)

F_PT = H * C
F_N1 = F_PT + 3 * H * PQ
F_N2 = F_N1 + HP
F_ALL = 384
G_PT = H * C
G_END = G_PT + 3 * H * PV
G_ALL = 512


def iota(shape, dim):
    return lax.broadcasted_iota(jnp.int32, shape, dim)


def head_of_feature(r):
    t = r - F_PT
    t = jnp.where(t >= 96, t - 96, jnp.where(t >= 48, t - 48, t))
    head = jnp.where(r < F_PT, r >> 4, t >> 2)
    head = jnp.where(r >= F_N1, r - F_N1, head)
    head = jnp.where(r >= F_N2, r - F_N2, head)
    return jnp.where(r >= F_N2 + HP, 99, head)


def head_of_value_feature(r):
    t = r - G_PT
    t = jnp.where(t >= 192, t - 192, jnp.where(t >= 96, t - 96, t))
    head = jnp.where(r < G_PT, r >> 4, t >> 3)
    return jnp.where(r >= G_END, 99, head)


def split2(x):
    hi = x.astype(BF16)
    return hi, (x - hi.astype(F32)).astype(BF16)


def split3(x):
    hi = x.astype(BF16)
    rest = x - hi.astype(F32)
    mid = rest.astype(BF16)
    return hi, mid, (rest - mid.astype(F32)).astype(BF16)


def mm(a, b):
    return jnp.dot(a, b, preferred_element_type=F32)


def mm_nt(a, b):
    return lax.dot_general(a, b, (((1,), (1,)), ((), ())), preferred_element_type=F32)


def softplus(x):
    return jnp.maximum(x, 0.0) + jnp.log(1.0 + jnp.exp(-jnp.abs(x)))


def coef_column(hw_ref, heads):
    coef = (0.5 * WL * WC) * softplus(hw_ref[...])
    rows = heads.shape[0]
    return jnp.sum(
        jnp.where(heads == iota((rows, H), 1), jnp.broadcast_to(coef, (rows, H)), 0.0),
        axis=1,
        keepdims=True,
    )


def rotate(rot, local, shift=None):
    out = []
    for x in range(3):
        t = rot[x][0] * local[0] + rot[x][1] * local[1] + rot[x][2] * local[2]
        out.append(t if shift is None else t + shift[x])
    return out


def pair_rows(head_rows, lane_block):
    keep = (iota(head_rows.shape, 0) >> 4) == lane_block
    return jnp.where(keep, head_rows, 0.0).astype(BF16)


def tile(k, size):
    return pl.ds(pl.multiple_of(k * size, size), size)


def mega(
    dims,
    pair_hbm,
    bw_ref,
    hw_ref,
    q_ref,
    k_ref,
    v_ref,
    qp_ref,
    kp_ref,
    vp_ref,
    rot_ref,
    tr_ref,
    count_ref,
    go_ref,
    gpt_ref,
    gpair_ref,
    pair_out,
    kfin_ref,
    qfin_ref,
    wfin_ref,
    pair_v,
    qf_s,
    kf_s,
    vf_s,
    gf_s,
    kt_s,
    kcat_s,
    qcat_s,
    vcat_s,
    gcat_s,
    kparts_s,
    vparts_s,
    w_s,
    g_s,
    p_s,
    pr_s,
    bias_s,
    ab_s,
    rhs_s,
    dh_s,
    dl_s,
    ah_s,
    al_s,
    qout_s,
    st_s,
    xst_s,
    cst_s,
    zst_s,
    sc_s,
    s0_s,
    sc0_s,
    s1_s,
    sy_s,
    s2_s,
    sr_s,
    v0_s,
    vc0_s,
    v1_s,
    vz_s,
    v2_s,
    vr_s,
    qx_s,
    qz_s,
    qr_s,
    wm_s,
    wx_s,
    wz_s,
    wc_s,
    wy_s,
    wr_s,
    pair_sem,
    out_sem,
    send_sem,
    recv_sem,
):
    nz, ny, nx, ni, nj = dims
    lanes = ni * HP
    groups = lanes // 128
    chunks = lanes // 256
    z, y, c = lax.axis_index("row_0"), lax.axis_index("row_1"), lax.axis_index("row_2")
    x, w = lax.axis_index("col_0"), lax.axis_index("col_1")

    for g in range(groups):
        pltpu.make_async_copy(
            pair_hbm.at[pl.ds(8 * g, 8)], pair_v.at[pl.ds(8 * g, 8)], pair_sem.at[g]
        ).start()

    barrier = pltpu.get_barrier_semaphore()
    peers = [{"row_2": 1 - c}, {"col_1": 1 - w}]
    peers += [{"row_1": lax.rem(y + r, ny)} for r in range(1, ny)]
    peers += [{"row_0": lax.rem(z + r, nz)} for r in range(1, nz)]
    peers += [{"col_0": lax.rem(x + r, nx)} for r in range(1, nx)]
    for peer in peers:
        pl.semaphore_signal(barrier, inc=1, device_id=peer, device_id_type=MESH)

    used = [0]

    def send(src, dst, peer):
        n = used[0]
        used[0] += 1
        copy = pltpu.make_async_remote_copy(
            src_ref=src,
            dst_ref=dst,
            send_sem=send_sem.at[n],
            recv_sem=recv_sem.at[n],
            device_id=peer,
            device_id_type=MESH,
        )
        copy.start()
        return copy

    base = pl.multiple_of((z * ny + y) * 128, 128)

    def own_half(full):
        return jnp.where(c == 1, pltpu.roll(full, 64, 1), full)[:, :ni]

    rot_q = []
    for a in range(3):
        t = own_half(rot_ref[a, :, pl.ds(base, 128)])
        rot_q.append([t[b : b + 1] for b in range(3)])
    t = own_half(tr_ref[:, pl.ds(base, 128)])
    tr_q = [t[a : a + 1] for a in range(3)]
    col = x * 2 + w
    kbase = tile(col, nj)
    rot_k = []
    for a in range(3):
        t = rot_ref[a, :, kbase]
        rot_k.append([t[b : b + 1] for b in range(3)])
    t = tr_ref[:, kbase]
    tr_k = [t[a : a + 1] for a in range(3)]

    norm_sel = ((iota((HP, 48), 1) >> 2) == iota((HP, 48), 0)).astype(F32)
    qg = rotate(rot_q, [qp_ref[b] for b in range(3)], tr_q)
    gg = rotate(rot_q, [jnp.transpose(gpt_ref[b]) for b in range(3)])
    qf_s[0:F_PT] = jnp.transpose(q_ref[...])
    for a in range(3):
        qf_s[F_PT + 48 * a : F_PT + 48 * (a + 1)] = qg[a]
    qf_s[F_N2 : F_N2 + HP] = jnp.ones((HP, ni), F32)
    qf_s[F_N1:F_N2] = jnp.dot(
        norm_sel, qg[0] * qg[0] + qg[1] * qg[1] + qg[2] * qg[2], precision=HIGHEST
    )
    qf_s[F_N2 + HP :] = jnp.zeros((F_ALL - F_N2 - HP, ni), F32)
    gf_s[0:G_PT] = jnp.transpose(go_ref[...])
    for a in range(3):
        gf_s[G_PT + 96 * a : G_PT + 96 * (a + 1)] = gg[a]
    gf_s[G_END:] = jnp.zeros((G_ALL - G_END, ni), F32)

    kg = rotate(rot_k, [kp_ref[b] for b in range(3)], tr_k)
    vg = rotate(rot_k, [vp_ref[b] for b in range(3)], tr_k)
    kf_s[0:F_PT] = k_ref[...]
    for a in range(3):
        kf_s[F_PT + 48 * a : F_PT + 48 * (a + 1)] = kg[a]
    kf_s[F_N2 : F_N2 + HP] = jnp.dot(
        norm_sel, kg[0] * kg[0] + kg[1] * kg[1] + kg[2] * kg[2], precision=HIGHEST
    )
    kf_s[F_N1:F_N2] = jnp.ones((HP, nj), F32)
    kf_s[F_N2 + HP :] = jnp.zeros((F_ALL - F_N2 - HP, nj), F32)
    vf_s[0:G_PT] = v_ref[...]
    for a in range(3):
        vf_s[G_PT + 96 * a : G_PT + 96 * (a + 1)] = vg[a]
    vf_s[G_END:] = jnp.zeros((G_ALL - G_END, nj), F32)

    r = iota((F_ALL, 1), 0)
    coef = coef_column(hw_ref, head_of_feature(r))
    scale = jnp.where(r < F_PT, WL * WS, jnp.where(r < F_N1, 2.0 * coef, -coef))
    kt = jnp.transpose(kf_s[...] * scale)
    kt_s[...] = kt
    hi, mid, lo = split3(kt)
    for n, part in enumerate((hi, hi, mid, mid, hi, lo)):
        kcat_s[:, F_ALL * n : F_ALL * (n + 1)] = part
    hi, lo = split2(jnp.transpose(vf_s[...]))
    for n, part in enumerate((hi, hi, lo)):
        vcat_s[:, G_ALL * n : G_ALL * (n + 1)] = part
    kparts_s[0], kparts_s[1] = split2(kf_s[...])
    vparts_s[0], vparts_s[1] = split2(vf_s[G_PT:G_END])

    q_parts = split3(qf_s[...])
    g_parts = split2(gf_s[...])

    def expand(n, _):
        lane = iota((ni, 256), 1)
        e = ((lane >> 4) + n * 16 == iota((ni, 256), 0)).astype(BF16)
        for b in range(F_ALL // 128):
            head = head_of_feature(iota((128, 256), 0) + 128 * b)
            keep = head == (iota((128, 256), 1) & 15)
            hi, mid, lo = [
                jnp.where(keep, mm(part[128 * b : 128 * (b + 1)], e), 0.0).astype(BF16)
                for part in q_parts
            ]
            for m, part in enumerate((hi, mid, hi, mid, lo, hi)):
                at = F_ALL * m + 128 * b
                qcat_s[at : at + 128, tile(n, 256)] = part
        for b in range(G_ALL // 128):
            head = head_of_value_feature(iota((128, 256), 0) + 128 * b)
            keep = head == (iota((128, 256), 1) & 15)
            hi, lo = [
                jnp.where(keep, mm(part[128 * b : 128 * (b + 1)], e), 0.0).astype(BF16)
                for part in g_parts
            ]
            for m, part in enumerate((hi, lo, hi)):
                at = G_ALL * m + 128 * b
                gcat_s[at : at + 128, tile(n, 256)] = part
        return 0

    lax.fori_loop(0, chunks, expand, 0)

    w_s[...] = jnp.zeros((HP, 128), F32)
    w_s[0:H] = bw_ref[...].astype(F32)
    g_s[...] = jnp.zeros((lanes, 128), F32)
    for b in range(H):
        g_s[pl.ds(b, ni, stride=HP), :] = gpair_ref[b].astype(F32)
    w_rows = jnp.concatenate([w_s[...]] * 8, axis=0)
    for b in range(8):
        rhs_s[0:128, 128 * b : 128 * (b + 1)] = pair_rows(w_rows, b)

    count = count_ref[0]

    def forward(n, _):
        t = tile(n, 256)
        p_s[:, t] = mm(kcat_s[...], qcat_s[:, t])
        pr_s[:, t] = mm(vcat_s[...], gcat_s[:, t])
        for half in range(2):
            g = 2 * n + half
            pltpu.make_async_copy(
                pair_hbm.at[pl.ds(8 * g, 8)], pair_v.at[pl.ds(8 * g, 8)], pair_sem.at[g]
            ).wait()
            g_rows = g_s[tile(g, 128)]
            for b in range(8):
                rhs_s[128:256, 128 * b : 128 * (b + 1)] = pair_rows(g_rows, b)
            acc = None
            for b in range(4):
                two = jnp.concatenate([pair_v[8 * g + 2 * b], pair_v[8 * g + 2 * b + 1]], axis=1)
                part = mm_nt(two, rhs_s[:, 256 * b : 256 * (b + 1)])
                acc = part if acc is None else acc + part
            bias_s[half] = acc
        first = col * nj
        peak = jnp.full((8, 256), -jnp.inf, F32)
        for b in range(0, nj, 32):
            rows = slice(b, b + 32)
            bias = jnp.concatenate([bias_s[0, rows, :128], bias_s[1, rows, :128]], axis=1)
            logits = p_s[rows, t] + WL * bias
            logits = jnp.where(iota((32, 256), 0) + (first + b) < count, logits, -1000000000.0)
            p_s[rows, t] = logits
            peak = jnp.maximum(peak, jnp.max(logits.reshape(4, 8, 256), axis=0))
        peak = jnp.max(peak, axis=0, keepdims=True)
        total = jnp.zeros((8, 256), F32)
        upper = jnp.zeros((8, 256), F32)
        for b in range(0, nj, 32):
            rows = slice(b, b + 32)
            more = jnp.concatenate([bias_s[0, rows, 128:], bias_s[1, rows, 128:]], axis=1)
            prod = pr_s[rows, t] + more
            e = jnp.exp(p_s[rows, t] - peak)
            pr_s[rows, t] = prod
            p_s[rows, t] = e
            total += jnp.sum(e.reshape(4, 8, 256), axis=0)
            upper += jnp.sum((e * prod).reshape(4, 8, 256), axis=0)
        total = jnp.sum(total, axis=0, keepdims=True)
        upper = jnp.sum(upper, axis=0, keepdims=True)
        for half in range(2):
            at = slice(128 * half, 128 * (half + 1))
            st_s[0, pl.ds(2 * n + half, 1), :] = peak[:, at]
            st_s[1, pl.ds(2 * n + half, 1), :] = total[:, at]
            st_s[2, pl.ds(2 * n + half, 1), :] = upper[:, at]
        return 0

    lax.fori_loop(0, chunks, forward, 0)

    pl.semaphore_wait(barrier, len(peers))
    copies = [send(st_s, xst_s.at[r - 1], {"col_0": lax.rem(x + r, nx)}) for r in range(1, nx)]
    for copy in copies:
        copy.wait()
    sets = [(st_s[0], st_s[1], st_s[2])]
    sets += [(xst_s[r, 0], xst_s[r, 1], xst_s[r, 2]) for r in range(nx - 1)]

    def merge(sets):
        peak = functools.reduce(jnp.maximum, [s[0] for s in sets])
        weights = [jnp.exp(s[0] - peak) for s in sets]
        total = sum(s[1] * f for s, f in zip(sets, weights))
        upper = sum(s[2] * f for s, f in zip(sets, weights))
        return peak, total, upper

    mine = merge(sets)
    for a in range(3):
        cst_s[a] = mine[a]
    send(cst_s, zst_s, {"col_1": 1 - w}).wait()
    peak, total, upper = merge([mine, (zst_s[0], zst_s[1], zst_s[2])])
    sc_s[0] = jnp.exp(st_s[0] - peak) / total
    sc_s[1] = upper / total

    def weights_of(g, acc):
        attn = p_s[:, tile(g, 128)] * sc_s[0, pl.ds(g, 1), :]
        dlog = attn * (pr_s[:, tile(g, 128)] - sc_s[1, pl.ds(g, 1), :])
        dh_s[:, tile(g, 128)], dl_s[:, tile(g, 128)] = split2(dlog)
        a_hi, a_lo = split2(attn)
        ah_s[:, tile(g, 128)] = a_hi
        al_s[:, tile(g, 128)] = a_lo
        scaled = WL * dlog
        ab_s[:, pl.ds(pl.multiple_of(g * 256, 256), 128)] = scaled.astype(BF16)
        ab_s[:, pl.ds(pl.multiple_of(g * 256 + 128, 128), 128)] = a_hi
        turned = jnp.transpose(dlog).astype(BF16)
        for b in range(8):
            acc = acc + mm(turned[16 * b : 16 * (b + 1)], pair_v[8 * g + b])
        return acc

    weight = lax.fori_loop(0, groups, weights_of, jnp.zeros((HP, 128), F32))

    slab = nj // (nz * ny * 2)

    def add(terms):
        return functools.reduce(lambda a, b: a + b, terms)

    def spread_to(src, dst, axis, me, count, slot):
        out = []
        for r in range(1, count):
            peer = lax.rem(me + r, count)
            out.append(send(src.at[slot(peer)], dst.at[r - 1], {axis: peer}))
        return out

    def done(copies):
        for copy in copies:
            copy.wait()

    kout = mm_nt(dh_s[...], qcat_s[0:F_ALL])
    kout += mm_nt(dh_s[...], qcat_s[F_ALL : 2 * F_ALL])
    kout += mm_nt(dl_s[...], qcat_s[0:F_ALL])
    s0_s[...] = kout.reshape(s0_s.shape)
    s_core = send(s0_s.at[:, :, 1 - c], sc0_s, {"row_2": 1 - c})
    spread = jnp.sum(kt_s[...] * kout, axis=0, keepdims=True)

    wm_s[0:H] = WL * weight[0:H]
    wm_s[H : H + 1] = spread[:, 128:256]
    wm_s[H + 1 : H + 2] = spread[:, 256:384]
    wm_s[H + 2 :] = jnp.zeros((HP - H - 2, 128), F32)

    def share(src, slots, axis, me, count):
        slots[me] = src[...]
        return [send(src, slots.at[me], {axis: lax.rem(me + r, count)}) for r in range(1, count)]

    def settle(copies, slots, dst, count):
        done(copies)
        dst[...] = add([slots[n] for n in range(count)])

    w_x = share(wm_s, wx_s, "col_0", x, nx)

    aout = mm_nt(ah_s[...], gcat_s[0:G_ALL])
    aout += mm_nt(ah_s[...], gcat_s[G_ALL : 2 * G_ALL])
    aout += mm_nt(al_s[...], gcat_s[0:G_ALL])
    v0_s[...] = aout.reshape(v0_s.shape)
    v_core = send(v0_s.at[:, :, 1 - c], vc0_s, {"row_2": 1 - c})

    s_core.wait()
    s1_s[...] = s0_s[:, :, c] + sc0_s[...]
    s_y = spread_to(s1_s, sy_s, "row_1", y, ny, lambda p: (slice(None), p))
    v_core.wait()
    v1_s[...] = v0_s[:, :, c] + vc0_s[...]
    settle(w_x, wx_s, wm_s, nx)
    w_w = send(wm_s, wz_s, {"col_1": 1 - w})
    v_z = spread_to(v1_s, vz_s, "row_0", z, nz, lambda p: p)

    qslab = ni // (nx * 2)
    first = used[0]
    used[0] += nx - 1

    def q_copy(r):
        peer = lax.rem(x + r, nx)
        return pltpu.make_async_remote_copy(
            src_ref=qout_s.at[peer],
            dst_ref=qx_s.at[r - 1],
            send_sem=send_sem.at[first + r - 1],
            recv_sem=recv_sem.at[first + r - 1],
            device_id={"col_0": peer},
            device_id_type=MESH,
        )

    def query_side(r, _):
        owner = lax.rem(x + r, nx)
        at = tile(owner, 256)
        e = ((iota((16, 256), 1) >> 4) == iota((16, 256), 0)).astype(BF16)
        his, los = [], []
        for parts, hi_ref, lo_ref, head_of, rows, start in (
            (kparts_s, dh_s, dl_s, head_of_feature, F_N2, 0),
            (vparts_s, ah_s, al_s, head_of_value_feature, G_END - G_PT, G_PT),
        ):
            full = mm(parts[0, 0:rows], hi_ref[:, at]) + mm(parts[0, 0:rows], lo_ref[:, at])
            full += mm(parts[1, 0:rows], hi_ref[:, at])
            keep = head_of(iota((rows, 256), 0) + start) == (iota((rows, 256), 1) & 15)
            hi, lo = split2(jnp.where(keep, full, 0.0))
            his.append(hi)
            los.append(lo)
        out = mm_nt(e, jnp.concatenate(his, axis=0)) + mm_nt(e, jnp.concatenate(los, axis=0))
        qout_s[owner] = out.reshape(2, qslab, qout_s.shape[3])

        @pl.when(r < nx)
        def _():
            q_copy(r).start()

        return 0

    lax.fori_loop(1, nx + 1, query_side, 0)

    def copy_out(g):
        at = pl.ds(pl.multiple_of(8 * g, 8), 8)
        return pltpu.make_async_copy(pair_v.at[at], pair_out.at[at], out_sem.at[g])

    def pair_group(g, _):
        g_rows = g_s[tile(g, 128)]
        for b in range(8):
            rhs_s[128:256, 128 * b : 128 * (b + 1)] = pair_rows(g_rows, b)
        for b in range(4):
            two = mm(ab_s[:, tile(g, 256)], rhs_s[:, 256 * b : 256 * (b + 1)]).astype(BF16)
            pair_v[8 * g + 2 * b] = two[:, :128]
            pair_v[8 * g + 2 * b + 1] = two[:, 128:]
        copy_out(g).start()
        return 0

    lax.fori_loop(0, groups // 2, pair_group, 0)
    w_w.wait()
    wm_s[...] = wm_s[...] + wz_s[...]
    w_c = send(wm_s, wc_s, {"row_2": 1 - c})
    done(s_y)
    s2_s[...] = add([s1_s[:, y]] + [sy_s[r] for r in range(ny - 1)])
    s_z = spread_to(s2_s, sr_s, "row_0", z, nz, lambda p: p)
    w_c.wait()
    wm_s[...] = wm_s[...] + wc_s[...]
    w_y = share(wm_s, wy_s, "row_1", y, ny)
    done(v_z)
    v2_s[...] = add([v1_s[z]] + [vz_s[r] for r in range(nz - 1)])
    v_y = spread_to(v2_s, vr_s, "row_1", y, ny, lambda p: p)
    done([q_copy(r) for r in range(1, nx)])
    qz_s[...] = add([qout_s[x]] + [qx_s[r] for r in range(nx - 1)])
    q_w = send(qz_s.at[1 - w], qr_s, {"col_1": 1 - w})
    lax.fori_loop(groups // 2, groups, pair_group, 0)
    settle(w_y, wy_s, wm_s, ny)
    w_z = share(wm_s, wr_s, "row_0", z, nz)
    done(s_z)
    kfin_ref[:, 0:F_ALL] = add([s2_s[z]] + [sr_s[r] for r in range(nz - 1)])
    done(v_y)
    kfin_ref[:, F_ALL:] = add([v2_s[y]] + [vr_s[r] for r in range(ny - 1)])
    q_w.wait()
    qfin_ref[...] = qz_s[w] + qr_s[...]
    settle(w_z, wr_s, wfin_ref, nz)
    for g in range(groups):
        copy_out(g).wait()


def finish(
    dims,
    pair_in,
    hw_ref,
    kfin_ref,
    qfin_ref,
    wfin_ref,
    qp_ref,
    kp_ref,
    vp_ref,
    rot_ref,
    tr_ref,
    gpt_ref,
    pair_out,
    q_out,
    qp_out,
    qf_out,
    k_out,
    v_out,
    kp_out,
    vp_out,
    kf_out,
    w_out,
    hw_out,
    t_s,
    pair_v,
    in_sem,
    out_sem,
):
    nz, ny, nx, ni, nj = dims
    z, y, c = lax.axis_index("row_0"), lax.axis_index("row_1"), lax.axis_index("row_2")
    x, w = lax.axis_index("col_0"), lax.axis_index("col_1")
    row = (z * ny + y) * 2 + c
    col = x * 2 + w
    slab = nj // (nz * ny * 2)
    qslab = ni // (nx * 2)

    groups = ni // 8

    def part(g, src, dst, sem):
        return pltpu.make_async_copy(src.at[pl.ds(8 * g, 8)], dst.at[pl.ds(8 * g, 8)], sem.at[g])

    for g in range(groups):
        part(g, pair_in, pair_v, in_sem).start()
    for g in range(groups):
        part(g, pair_in, pair_v, in_sem).wait()
        part(g, pair_v, pair_out, out_sem).start()

    def exact(a, b):
        return jnp.dot(a, b, precision=HIGHEST)

    def from_lane(rows, at):
        return pltpu.roll(rows, lax.rem(128 - at, 128), 1)

    def over(t):
        return jnp.sum(t, axis=1, keepdims=True)

    def columns(t):
        return [[t[:, 3 * a + b : 3 * a + b + 1] for b in range(3)] for a in range(3)]

    def back(rot, v):
        return [rot[0][b] * v[0] + rot[1][b] * v[1] + rot[2][b] * v[2] for b in range(3)]

    def frame(out, cols, count):
        t = jnp.zeros((count, 128), F32)
        for n in range(12):
            t = jnp.where(iota((count, 128), 1) == n, cols[n // 4][n % 4], t)
        t_s[0:count] = t
        turned = jnp.transpose(t_s[0:128])
        for a in range(3):
            out[a] = turned[4 * a : 4 * a + 4, :count]

    expand = (iota((HP, 48), 0) == (iota((HP, 48), 1) >> 2)).astype(F32)
    coef = jnp.broadcast_to(coef_column(hw_ref, iota((48, 1), 0) >> 2), (48, 48))
    coef = jnp.where(iota((48, 48), 0) == iota((48, 48), 1), coef, 0.0)
    coef = jnp.sum(coef, axis=0, keepdims=True)

    t_s[...] = jnp.zeros(t_s.shape, F32)
    at = row * slab
    base = tile(col * (nj // 128) + at // 128, 128)
    here = tile(at // 128, 128)
    for a in range(3):
        t_s[3 * a : 3 * a + 3] = rot_ref[a, :, base]
        t_s[16 + 48 * a : 16 + 48 * (a + 1)] = kp_ref[a, :, here]
        t_s[160 + 96 * a : 160 + 96 * (a + 1)] = vp_ref[a, :, here]
    t_s[9:12] = tr_ref[:, base]
    own = jnp.transpose(from_lane(t_s[...], lax.rem(at, 128)))[:slab]
    rot = columns(own)
    shift = [own[:, 9 + a : 10 + a] for a in range(3)]
    kp = [own[:, 16 + 48 * b : 16 + 48 * (b + 1)] for b in range(3)]
    vp = [own[:, 160 + 96 * b : 160 + 96 * (b + 1)] for b in range(3)]
    kg = rotate(rot, kp, shift)
    k_out[...] = (WL * WS) * kfin_ref[:, 0:F_PT]
    v_out[...] = kfin_ref[:, F_ALL : F_ALL + G_PT]
    sums = exact(kfin_ref[:, F_N2 : F_N2 + HP], expand)
    dkg = []
    for a in range(3):
        piece = kfin_ref[:, F_PT + 48 * a : F_PT + 48 * (a + 1)]
        dkg.append(2.0 * coef * (piece - kg[a] * sums))
    v_at = F_ALL + G_PT
    dvg = [kfin_ref[:, v_at + 96 * a : v_at + 96 * (a + 1)] for a in range(3)]
    for b, (dk, dv) in enumerate(zip(back(rot, dkg), back(rot, dvg))):
        kp_out[b] = dk
        vp_out[b] = dv
    cols = []
    for a in range(3):
        cols.append([over(dkg[a] * kp[b]) + over(dvg[a] * vp[b]) for b in range(3)])
        cols[a].append(over(dkg[a]) + over(dvg[a]))
    frame(kf_out, cols, slab)

    at = col * qslab
    base = tile(z * ny + y, 128)
    t_s[...] = jnp.zeros(t_s.shape, F32)
    for a in range(3):
        t_s[3 * a : 3 * a + 3] = rot_ref[a, :, base]
        t_s[16 + 48 * a : 16 + 48 * (a + 1), 0:ni] = qp_ref[a]
    t_s[9:12] = tr_ref[:, base]
    t_s[0:16] = from_lane(t_s[0:16], c * ni + at)
    t_s[16:160] = from_lane(t_s[16:160], at)
    own = jnp.transpose(t_s[0:256])[:qslab]
    rot = columns(own)
    shift = [own[:, 9 + a : 10 + a] for a in range(3)]
    qp = [own[:, 16 + 48 * b : 16 + 48 * (b + 1)] for b in range(3)]
    gp = [gpt_ref[b, tile(col, qslab), :] for b in range(3)]
    qg = rotate(rot, qp, shift)
    gg = rotate(rot, gp)
    q_out[...] = (WL * WS) * qfin_ref[:, 0:F_PT]
    sums = exact(qfin_ref[:, F_N1:F_N2], expand)
    dqg = []
    for a in range(3):
        piece = qfin_ref[:, F_PT + 48 * a : F_PT + 48 * (a + 1)]
        dqg.append(-2.0 * coef * (qg[a] * sums - piece))
    opt = [qfin_ref[:, F_N2 + 96 * a : F_N2 + 96 * (a + 1)] - shift[a] for a in range(3)]
    for b, dq in enumerate(back(rot, dqg)):
        qp_out[b] = dq
    cols = []
    for a in range(3):
        cols.append([over(dqg[a] * qp[b]) + over(opt[a] * gp[b]) for b in range(3)])
        cols[a].append(over(dqg[a]) - over(gg[a]))
    frame(qf_out, cols, qslab)

    w_out[...] = wfin_ref[0:H]
    total = jnp.zeros((1, 128), F32)
    for n in range(2):
        f = iota((128, 128), 0) + 128 * (n + 1)
        keep = (head_of_feature(f) == iota((128, 128), 1)) & (f >= F_PT)
        total += exact(wfin_ref[H + n : H + n + 1], keep.astype(F32))
    hw = hw_ref[...]
    hw_out[...] = total[:, 0:H] / (softplus(hw) * (1.0 + jnp.exp(-hw)))

    for g in range(groups):
        part(g, pair_v, pair_out, out_sem).wait()


def per_device(dims, *args):
    (pair, bw, hw, q, k, v, qp, kp, vp, rot, tr, count, go, gpt, gpair) = args
    nz, ny, nx, ni, nj = dims
    hw = hw.reshape(1, H)
    bw, q, go = bw.T, q.T, go.T
    gpt = jnp.transpose(gpt, (0, 2, 1))
    gpair = jnp.transpose(gpair, (1, 0, 2))
    lanes = ni * HP
    slab, qslab = nj // (nz * ny * 2), ni // (nx * 2)
    kw, qw = F_ALL + G_ALL, F_N2 + G_END - G_PT
    groups = lanes // 128
    sends = 3 * nx + 3 * (ny - 1) + 3 * (nz - 1) + 3

    def buf(*shape, dtype=F32):
        return pltpu.VMEM(shape, dtype)

    pair_grad, kfin, qfin, wfin = pl.pallas_call(
        functools.partial(mega, dims),
        out_shape=[
            jax.ShapeDtypeStruct((ni, nj, CZ), BF16),
            jax.ShapeDtypeStruct((slab, kw), F32),
            jax.ShapeDtypeStruct((qslab, qw), F32),
            jax.ShapeDtypeStruct((HP, 128), F32),
        ],
        in_specs=[ANY] + [VMEM] * 10 + [SMEM] + [VMEM] * 3,
        out_specs=[ANY] + [VMEM] * 3,
        scratch_shapes=[
            buf(ni, nj, CZ, dtype=BF16),
            buf(F_ALL, ni),
            buf(F_ALL, nj),
            buf(G_ALL, nj),
            buf(G_ALL, ni),
            buf(nj, F_ALL),
            buf(nj, 6 * F_ALL, dtype=BF16),
            buf(6 * F_ALL, lanes, dtype=BF16),
            buf(nj, 3 * G_ALL, dtype=BF16),
            buf(3 * G_ALL, lanes, dtype=BF16),
            buf(2, F_ALL, nj, dtype=BF16),
            buf(2, G_END - G_PT, nj, dtype=BF16),
            buf(HP, 128),
            buf(lanes, 128),
            buf(nj, lanes),
            buf(nj, lanes),
            buf(2, nj, 256),
            buf(nj, 2 * lanes, dtype=BF16),
            buf(256, 1024, dtype=BF16),
            buf(nj, lanes, dtype=BF16),
            buf(nj, lanes, dtype=BF16),
            buf(nj, lanes, dtype=BF16),
            buf(nj, lanes, dtype=BF16),
            buf(nx, 2, qslab, qw),
            buf(3, groups, 128),
            buf(nx - 1, 3, groups, 128),
            buf(3, groups, 128),
            buf(3, groups, 128),
            buf(2, groups, 128),
            buf(nz, ny, 2, slab, F_ALL),
            buf(nz, ny, slab, F_ALL),
            buf(nz, ny, slab, F_ALL),
            buf(ny - 1, nz, slab, F_ALL),
            buf(nz, slab, F_ALL),
            buf(nz - 1, slab, F_ALL),
            buf(nz, ny, 2, slab, G_ALL),
            buf(nz, ny, slab, G_ALL),
            buf(nz, ny, slab, G_ALL),
            buf(nz - 1, ny, slab, G_ALL),
            buf(ny, slab, G_ALL),
            buf(ny - 1, slab, G_ALL),
            buf(nx - 1, 2, qslab, qw),
            buf(2, qslab, qw),
            buf(qslab, qw),
            buf(HP, 128),
            buf(nx, HP, 128),
            buf(HP, 128),
            buf(HP, 128),
            buf(ny, HP, 128),
            buf(nz, HP, 128),
            pltpu.SemaphoreType.DMA((groups,)),
            pltpu.SemaphoreType.DMA((groups,)),
            pltpu.SemaphoreType.DMA((sends,)),
            pltpu.SemaphoreType.DMA((sends,)),
        ],
        compiler_params=pltpu.CompilerParams(
            collective_id=0, has_side_effects=True, vmem_limit_bytes=60 * 2**20
        ),
        name="tile_and_reduce",
    )(pair, bw, hw, q, k, v, qp, kp, vp, rot, tr, count, go, gpt, gpair)

    outs = [
        jax.ShapeDtypeStruct((ni, nj, CZ), BF16),
        jax.ShapeDtypeStruct((qslab, H * C), F32),
        jax.ShapeDtypeStruct((3, qslab, H * PQ), F32),
        jax.ShapeDtypeStruct((3, 4, qslab), F32),
        jax.ShapeDtypeStruct((slab, H * C), F32),
        jax.ShapeDtypeStruct((slab, H * C), F32),
        jax.ShapeDtypeStruct((3, slab, H * PQ), F32),
        jax.ShapeDtypeStruct((3, slab, H * PV), F32),
        jax.ShapeDtypeStruct((3, 4, slab), F32),
        jax.ShapeDtypeStruct((H, CZ), F32),
        jax.ShapeDtypeStruct((1, H), F32),
    ]
    small = [hw, kfin, qfin, wfin, qp, kp, vp, rot, tr, gpt]
    res = pl.pallas_call(
        functools.partial(finish, dims),
        out_shape=outs,
        in_specs=[ANY] + [VMEM] * 10,
        out_specs=[ANY] + [VMEM] * 10,
        scratch_shapes=[
            buf(512, 128),
            buf(ni, nj, CZ, dtype=BF16),
            pltpu.SemaphoreType.DMA((groups,)),
            pltpu.SemaphoreType.DMA((groups,)),
        ],
        compiler_params=pltpu.CompilerParams(vmem_limit_bytes=60 * 2**20),
        name="pair_and_frames",
    )(pair_grad, *small)
    pair_grad, dq, dqp, dqf, dk, dv, dkp, dvp, dkf, dw, dhw = res
    turn = functools.partial(jnp.transpose, axes=(0, 2, 1))
    return pair_grad, dq.T, turn(dqp), dqf, dk.T, dv.T, turn(dkp), turn(dvp), dkf, dw.T, dhw[0]


def solution(mesh):
    finer = Mesh(mesh.devices.reshape(4, 4, 2, 4, 2), ("row_0", "row_1", "row_2", "col_0", "col_1"))
    return sharded(finer, 64, 256)


def sharded(finer, ni, nj):
    sizes = finer.shape
    dims = (sizes["row_0"], sizes["row_1"], sizes["col_0"], ni, nj)
    in_specs = (
        P(ROW, COL, None),
        P(),
        P(),
        P(None, ROW),
        P(None, COL),
        P(None, COL),
        P(None, None, ROW),
        P(None, None, COL),
        P(None, None, COL),
        P(),
        P(),
        P(),
        P(None, ROW),
        P(None, None, ROW),
        P(ROW, None, None),
    )
    out_specs = (
        P(ROW, COL, None),
        P(None, ROW_COL),
        P(None, None, ROW_COL),
        P(None, None, ROW_COL),
        P(None, COL_ROW),
        P(None, COL_ROW),
        P(None, None, COL_ROW),
        P(None, None, COL_ROW),
        P(None, None, COL_ROW),
        P(),
        P(),
    )
    return jax.shard_map(
        functools.partial(per_device, dims),
        mesh=finer,
        in_specs=in_specs,
        out_specs=out_specs,
        check_vma=False,
    )
```

```python
import functools
import math

import jax
import jax.numpy as jnp
from jax import lax
from jax.experimental import pallas as pl
from jax.experimental.pallas import tpu as pltpu
from jax.sharding import Mesh
from jax.sharding import PartitionSpec as P

ROW = ("row_0", "row_1", "row_2")
COL = ("col_0", "col_1")
ROW_COL = ("row_0", "row_1", "row_2", "col_0", "col_1")
COL_ROW = ("col_0", "col_1", "row_0", "row_1", "row_2")

MESH = pl.DeviceIdType.MESH
HIGHEST = lax.Precision.HIGHEST
F32 = jnp.float32
BF16 = jnp.bfloat16
VMEM = pl.BlockSpec(memory_space=pltpu.VMEM)
ANY = pl.BlockSpec(memory_space=pl.ANY)
SMEM = pl.BlockSpec(memory_space=pltpu.SMEM)

H, C, PQ, PV, CZ = 12, 16, 4, 8, 128
HP = 16
WL = math.sqrt(1.0 / 3.0)
WC = math.sqrt(2.0 / (9.0 * PQ))
WS = 1.0 / math.sqrt(C)

F_PT = H * C
F_N1 = F_PT + 3 * H * PQ
F_N2 = F_N1 + HP
F_ALL = 384
G_PT = H * C
G_END = G_PT + 3 * H * PV
G_ALL = 512


def iota(shape, dim):
    return lax.broadcasted_iota(jnp.int32, shape, dim)


def head_of_feature(r):
    t = r - F_PT
    t = jnp.where(t >= 96, t - 96, jnp.where(t >= 48, t - 48, t))
    head = jnp.where(r < F_PT, r >> 4, t >> 2)
    head = jnp.where(r >= F_N1, r - F_N1, head)
    head = jnp.where(r >= F_N2, r - F_N2, head)
    return jnp.where(r >= F_N2 + HP, 99, head)


def head_of_value_feature(r):
    t = r - G_PT
    t = jnp.where(t >= 192, t - 192, jnp.where(t >= 96, t - 96, t))
    head = jnp.where(r < G_PT, r >> 4, t >> 3)
    return jnp.where(r >= G_END, 99, head)


def split2(x):
    hi = x.astype(BF16)
    return hi, (x - hi.astype(F32)).astype(BF16)


def split3(x):
    hi = x.astype(BF16)
    rest = x - hi.astype(F32)
    mid = rest.astype(BF16)
    return hi, mid, (rest - mid.astype(F32)).astype(BF16)


def mm(a, b):
    return jnp.dot(a, b, preferred_element_type=F32)


def mm_nt(a, b):
    return lax.dot_general(a, b, (((1,), (1,)), ((), ())), preferred_element_type=F32)


def softplus(x):
    return jnp.maximum(x, 0.0) + jnp.log(1.0 + jnp.exp(-jnp.abs(x)))


def coef_column(hw_ref, heads):
    coef = (0.5 * WL * WC) * softplus(hw_ref[...])
    rows = heads.shape[0]
    return jnp.sum(
        jnp.where(heads == iota((rows, H), 1), jnp.broadcast_to(coef, (rows, H)), 0.0),
        axis=1,
        keepdims=True,
    )


def rotate(rot, local, shift=None):
    out = []
    for x in range(3):
        t = rot[x][0] * local[0] + rot[x][1] * local[1] + rot[x][2] * local[2]
        out.append(t if shift is None else t + shift[x])
    return out


def pair_rows(head_rows, lane_block):
    keep = (iota(head_rows.shape, 0) >> 4) == lane_block
    return jnp.where(keep, head_rows, 0.0).astype(BF16)


def tile(k, size):
    return pl.ds(pl.multiple_of(k * size, size), size)


def mega(
    dims,
    pair_hbm,
    bw_ref,
    hw_ref,
    q_ref,
    k_ref,
    v_ref,
    qp_ref,
    kp_ref,
    vp_ref,
    rot_ref,
    tr_ref,
    count_ref,
    go_ref,
    gpt_ref,
    gpair_ref,
    pair_out,
    kfin_ref,
    qfin_ref,
    wfin_ref,
    pair_v,
    qf_s,
    kf_s,
    vf_s,
    gf_s,
    kt_s,
    kcat_s,
    qcat_s,
    vcat_s,
    gcat_s,
    kparts_s,
    vparts_s,
    w_s,
    g_s,
    p_s,
    pr_s,
    bias_s,
    ab_s,
    rhs_s,
    dh_s,
    dl_s,
    ah_s,
    al_s,
    qout_s,
    st_s,
    xst_s,
    cst_s,
    zst_s,
    sc_s,
    s0_s,
    sc0_s,
    s1_s,
    sa_s,
    s2_s,
    sr_s,
    v0_s,
    vc0_s,
    v1_s,
    va_s,
    v2_s,
    vr_s,
    qx_s,
    qz_s,
    qr_s,
    wm_s,
    wx_s,
    wz_s,
    wc_s,
    wy_s,
    wr_s,
    pair_sem,
    out_sem,
    send_sem,
    recv_sem,
):
    nz, ny, nx, ni, nj = dims
    lanes = ni * HP
    groups = lanes // 128
    chunks = lanes // 256
    z, y, c = lax.axis_index("row_0"), lax.axis_index("row_1"), lax.axis_index("row_2")
    x, w = lax.axis_index("col_0"), lax.axis_index("col_1")

    for g in range(groups):
        pltpu.make_async_copy(
            pair_hbm.at[pl.ds(8 * g, 8)], pair_v.at[pl.ds(8 * g, 8)], pair_sem.at[g]
        ).start()

    barrier = pltpu.get_barrier_semaphore()
    peers = [{"row_2": 1 - c}, {"col_1": 1 - w}]
    peers += [{"row_1": lax.rem(y + r, ny)} for r in range(1, ny)]
    peers += [{"row_0": lax.rem(z + r, nz)} for r in range(1, nz)]
    peers += [{"col_0": lax.rem(x + r, nx)} for r in range(1, nx)]
    for peer in peers:
        pl.semaphore_signal(barrier, inc=1, device_id=peer, device_id_type=MESH)

    used = [0]

    def send(src, dst, peer):
        n = used[0]
        used[0] += 1
        copy = pltpu.make_async_remote_copy(
            src_ref=src,
            dst_ref=dst,
            send_sem=send_sem.at[n],
            recv_sem=recv_sem.at[n],
            device_id=peer,
            device_id_type=MESH,
        )
        copy.start()
        return copy

    base = pl.multiple_of((z * ny + y) * 128, 128)

    def own_half(full):
        return jnp.where(c == 1, pltpu.roll(full, 64, 1), full)[:, :ni]

    rot_q = []
    for a in range(3):
        t = own_half(rot_ref[a, :, pl.ds(base, 128)])
        rot_q.append([t[b : b + 1] for b in range(3)])
    t = own_half(tr_ref[:, pl.ds(base, 128)])
    tr_q = [t[a : a + 1] for a in range(3)]
    col = x * 2 + w
    kbase = tile(col, nj)
    rot_k = []
    for a in range(3):
        t = rot_ref[a, :, kbase]
        rot_k.append([t[b : b + 1] for b in range(3)])
    t = tr_ref[:, kbase]
    tr_k = [t[a : a + 1] for a in range(3)]

    norm_sel = ((iota((HP, 48), 1) >> 2) == iota((HP, 48), 0)).astype(F32)
    qg = rotate(rot_q, [qp_ref[b] for b in range(3)], tr_q)
    gg = rotate(rot_q, [jnp.transpose(gpt_ref[b]) for b in range(3)])
    qf_s[0:F_PT] = jnp.transpose(q_ref[...])
    for a in range(3):
        qf_s[F_PT + 48 * a : F_PT + 48 * (a + 1)] = qg[a]
    qf_s[F_N2 : F_N2 + HP] = jnp.ones((HP, ni), F32)
    qf_s[F_N1:F_N2] = jnp.dot(
        norm_sel, qg[0] * qg[0] + qg[1] * qg[1] + qg[2] * qg[2], precision=HIGHEST
    )
    qf_s[F_N2 + HP :] = jnp.zeros((F_ALL - F_N2 - HP, ni), F32)
    gf_s[0:G_PT] = jnp.transpose(go_ref[...])
    for a in range(3):
        gf_s[G_PT + 96 * a : G_PT + 96 * (a + 1)] = gg[a]
    gf_s[G_END:] = jnp.zeros((G_ALL - G_END, ni), F32)

    kg = rotate(rot_k, [kp_ref[b] for b in range(3)], tr_k)
    vg = rotate(rot_k, [vp_ref[b] for b in range(3)], tr_k)
    kf_s[0:F_PT] = k_ref[...]
    for a in range(3):
        kf_s[F_PT + 48 * a : F_PT + 48 * (a + 1)] = kg[a]
    kf_s[F_N2 : F_N2 + HP] = jnp.dot(
        norm_sel, kg[0] * kg[0] + kg[1] * kg[1] + kg[2] * kg[2], precision=HIGHEST
    )
    kf_s[F_N1:F_N2] = jnp.ones((HP, nj), F32)
    kf_s[F_N2 + HP :] = jnp.zeros((F_ALL - F_N2 - HP, nj), F32)
    vf_s[0:G_PT] = v_ref[...]
    for a in range(3):
        vf_s[G_PT + 96 * a : G_PT + 96 * (a + 1)] = vg[a]
    vf_s[G_END:] = jnp.zeros((G_ALL - G_END, nj), F32)

    r = iota((F_ALL, 1), 0)
    coef = coef_column(hw_ref, head_of_feature(r))
    scale = jnp.where(r < F_PT, WL * WS, jnp.where(r < F_N1, 2.0 * coef, -coef))
    kt = jnp.transpose(kf_s[...] * scale)
    kt_s[...] = kt
    hi, mid, lo = split3(kt)
    for n, part in enumerate((hi, hi, mid, mid, hi, lo)):
        kcat_s[:, F_ALL * n : F_ALL * (n + 1)] = part
    hi, lo = split2(jnp.transpose(vf_s[...]))
    for n, part in enumerate((hi, hi, lo)):
        vcat_s[:, G_ALL * n : G_ALL * (n + 1)] = part
    kparts_s[0], kparts_s[1] = split2(kf_s[...])
    vparts_s[0], vparts_s[1] = split2(vf_s[G_PT:G_END])

    q_parts = split3(qf_s[...])
    g_parts = split2(gf_s[...])

    def expand(n, _):
        lane = iota((ni, 256), 1)
        e = ((lane >> 4) + n * 16 == iota((ni, 256), 0)).astype(BF16)
        for b in range(F_ALL // 128):
            head = head_of_feature(iota((128, 256), 0) + 128 * b)
            keep = head == (iota((128, 256), 1) & 15)
            hi, mid, lo = [
                jnp.where(keep, mm(part[128 * b : 128 * (b + 1)], e), 0.0).astype(BF16)
                for part in q_parts
            ]
            for m, part in enumerate((hi, mid, hi, mid, lo, hi)):
                at = F_ALL * m + 128 * b
                qcat_s[at : at + 128, tile(n, 256)] = part
        for b in range(G_ALL // 128):
            head = head_of_value_feature(iota((128, 256), 0) + 128 * b)
            keep = head == (iota((128, 256), 1) & 15)
            hi, lo = [
                jnp.where(keep, mm(part[128 * b : 128 * (b + 1)], e), 0.0).astype(BF16)
                for part in g_parts
            ]
            for m, part in enumerate((hi, lo, hi)):
                at = G_ALL * m + 128 * b
                gcat_s[at : at + 128, tile(n, 256)] = part
        return 0

    lax.fori_loop(0, chunks, expand, 0)

    w_s[...] = jnp.zeros((HP, 128), F32)
    w_s[0:H] = bw_ref[...].astype(F32)
    g_s[...] = jnp.zeros((lanes, 128), F32)
    for b in range(H):
        g_s[pl.ds(b, ni, stride=HP), :] = gpair_ref[b].astype(F32)
    w_rows = jnp.concatenate([w_s[...]] * 8, axis=0)
    for b in range(8):
        rhs_s[0:128, 128 * b : 128 * (b + 1)] = pair_rows(w_rows, b)

    count = count_ref[0]

    def forward(n, _):
        t = tile(n, 256)
        p_s[:, t] = mm(kcat_s[...], qcat_s[:, t])
        pr_s[:, t] = mm(vcat_s[...], gcat_s[:, t])
        for half in range(2):
            g = 2 * n + half
            pltpu.make_async_copy(
                pair_hbm.at[pl.ds(8 * g, 8)], pair_v.at[pl.ds(8 * g, 8)], pair_sem.at[g]
            ).wait()
            g_rows = g_s[tile(g, 128)]
            for b in range(8):
                rhs_s[128:256, 128 * b : 128 * (b + 1)] = pair_rows(g_rows, b)
            acc = None
            for b in range(4):
                two = jnp.concatenate([pair_v[8 * g + 2 * b], pair_v[8 * g + 2 * b + 1]], axis=1)
                part = mm_nt(two, rhs_s[:, 256 * b : 256 * (b + 1)])
                acc = part if acc is None else acc + part
            bias_s[half] = acc
        first = col * nj
        peak = jnp.full((8, 256), -jnp.inf, F32)
        for b in range(0, nj, 32):
            rows = slice(b, b + 32)
            bias = jnp.concatenate([bias_s[0, rows, :128], bias_s[1, rows, :128]], axis=1)
            logits = p_s[rows, t] + WL * bias
            logits = jnp.where(iota((32, 256), 0) + (first + b) < count, logits, -1000000000.0)
            p_s[rows, t] = logits
            peak = jnp.maximum(peak, jnp.max(logits.reshape(4, 8, 256), axis=0))
        peak = jnp.max(peak, axis=0, keepdims=True)
        total = jnp.zeros((8, 256), F32)
        upper = jnp.zeros((8, 256), F32)
        for b in range(0, nj, 32):
            rows = slice(b, b + 32)
            more = jnp.concatenate([bias_s[0, rows, 128:], bias_s[1, rows, 128:]], axis=1)
            prod = pr_s[rows, t] + more
            e = jnp.exp(p_s[rows, t] - peak)
            pr_s[rows, t] = prod
            p_s[rows, t] = e
            total += jnp.sum(e.reshape(4, 8, 256), axis=0)
            upper += jnp.sum((e * prod).reshape(4, 8, 256), axis=0)
        total = jnp.sum(total, axis=0, keepdims=True)
        upper = jnp.sum(upper, axis=0, keepdims=True)
        for half in range(2):
            at = slice(128 * half, 128 * (half + 1))
            st_s[0, pl.ds(2 * n + half, 1), :] = peak[:, at]
            st_s[1, pl.ds(2 * n + half, 1), :] = total[:, at]
            st_s[2, pl.ds(2 * n + half, 1), :] = upper[:, at]
        return 0

    lax.fori_loop(0, chunks, forward, 0)

    pl.semaphore_wait(barrier, len(peers))
    copies = [send(st_s, xst_s.at[r - 1], {"col_0": lax.rem(x + r, nx)}) for r in range(1, nx)]
    for copy in copies:
        copy.wait()
    sets = [(st_s[0], st_s[1], st_s[2])]
    sets += [(xst_s[r, 0], xst_s[r, 1], xst_s[r, 2]) for r in range(nx - 1)]

    def merge(sets):
        peak = functools.reduce(jnp.maximum, [s[0] for s in sets])
        weights = [jnp.exp(s[0] - peak) for s in sets]
        total = sum(s[1] * f for s, f in zip(sets, weights))
        upper = sum(s[2] * f for s, f in zip(sets, weights))
        return peak, total, upper

    mine = merge(sets)
    for a in range(3):
        cst_s[a] = mine[a]
    send(cst_s, zst_s, {"col_1": 1 - w}).wait()
    peak, total, upper = merge([mine, (zst_s[0], zst_s[1], zst_s[2])])
    sc_s[0] = jnp.exp(st_s[0] - peak) / total
    sc_s[1] = upper / total

    def weights_of(g, acc):
        attn = p_s[:, tile(g, 128)] * sc_s[0, pl.ds(g, 1), :]
        dlog = attn * (pr_s[:, tile(g, 128)] - sc_s[1, pl.ds(g, 1), :])
        dh_s[:, tile(g, 128)], dl_s[:, tile(g, 128)] = split2(dlog)
        a_hi, a_lo = split2(attn)
        ah_s[:, tile(g, 128)] = a_hi
        al_s[:, tile(g, 128)] = a_lo
        scaled = WL * dlog
        ab_s[:, pl.ds(pl.multiple_of(g * 256, 256), 128)] = scaled.astype(BF16)
        ab_s[:, pl.ds(pl.multiple_of(g * 256 + 128, 128), 128)] = a_hi
        turned = jnp.transpose(dlog).astype(BF16)
        for b in range(8):
            acc = acc + mm(turned[16 * b : 16 * (b + 1)], pair_v[8 * g + b])
        return acc

    weight = lax.fori_loop(0, groups, weights_of, jnp.zeros((HP, 128), F32))

    slab = nj // (nz * ny * 2)

    def add(terms):
        return functools.reduce(lambda a, b: a + b, terms)

    def spread_to(src, dst, axis, me, count, slot):
        out = []
        for r in range(1, count):
            peer = lax.rem(me + r, count)
            out.append(send(src.at[slot(peer)], dst.at[r - 1], {axis: peer}))
        return out

    def done(copies):
        for copy in copies:
            copy.wait()

    kout = mm_nt(dh_s[...], qcat_s[0:F_ALL])
    kout += mm_nt(dh_s[...], qcat_s[F_ALL : 2 * F_ALL])
    kout += mm_nt(dl_s[...], qcat_s[0:F_ALL])
    s0_s[...] = kout.reshape(s0_s.shape)
    s_core = send(s0_s.at[:, :, 1 - c], sc0_s, {"row_2": 1 - c})
    spread = jnp.sum(kt_s[...] * kout, axis=0, keepdims=True)

    wm_s[0:H] = WL * weight[0:H]
    wm_s[H : H + 1] = spread[:, 128:256]
    wm_s[H + 1 : H + 2] = spread[:, 256:384]
    wm_s[H + 2 :] = jnp.zeros((HP - H - 2, 128), F32)

    def share(src, slots, axis, me, count):
        slots[me] = src[...]
        return [send(src, slots.at[me], {axis: lax.rem(me + r, count)}) for r in range(1, count)]

    def settle(copies, slots, dst, count):
        done(copies)
        dst[...] = add([slots[n] for n in range(count)])

    w_c = send(wm_s, wc_s, {"row_2": 1 - c})

    aout = mm_nt(ah_s[...], gcat_s[0:G_ALL])
    aout += mm_nt(ah_s[...], gcat_s[G_ALL : 2 * G_ALL])
    aout += mm_nt(al_s[...], gcat_s[0:G_ALL])
    v0_s[...] = aout.reshape(v0_s.shape)
    v_core = send(v0_s.at[:, :, 1 - c], vc0_s, {"row_2": 1 - c})

    w_c.wait()
    wm_s[...] = wm_s[...] + wc_s[...]
    w_x = share(wm_s, wx_s, "col_0", x, nx)
    qslab = ni // (nx * 2)
    first = used[0]
    used[0] += nx - 1

    def q_copy(r):
        peer = lax.rem(x + r, nx)
        return pltpu.make_async_remote_copy(
            src_ref=qout_s.at[peer],
            dst_ref=qx_s.at[r - 1],
            send_sem=send_sem.at[first + r - 1],
            recv_sem=recv_sem.at[first + r - 1],
            device_id={"col_0": peer},
            device_id_type=MESH,
        )

    def query_side(r, _):
        owner = lax.rem(x + r, nx)
        at = tile(owner, 256)
        e = ((iota((16, 256), 1) >> 4) == iota((16, 256), 0)).astype(BF16)
        his, los = [], []
        for parts, hi_ref, lo_ref, head_of, rows, start in (
            (kparts_s, dh_s, dl_s, head_of_feature, F_N2, 0),
            (vparts_s, ah_s, al_s, head_of_value_feature, G_END - G_PT, G_PT),
        ):
            full = mm(parts[0, 0:rows], hi_ref[:, at]) + mm(parts[0, 0:rows], lo_ref[:, at])
            full += mm(parts[1, 0:rows], hi_ref[:, at])
            keep = head_of(iota((rows, 256), 0) + start) == (iota((rows, 256), 1) & 15)
            hi, lo = split2(jnp.where(keep, full, 0.0))
            his.append(hi)
            los.append(lo)
        out = mm_nt(e, jnp.concatenate(his, axis=0)) + mm_nt(e, jnp.concatenate(los, axis=0))
        qout_s[owner] = out.reshape(2, qslab, qout_s.shape[3])

        @pl.when(r < nx)
        def _():
            q_copy(r).start()

        return 0

    lax.fori_loop(1, 1 + nx // 2, query_side, 0)
    s_core.wait()
    s1_s[...] = s0_s[:, :, c] + sc0_s[...]
    s_first = spread_to(s1_s, sa_s, "row_0", z, nz, lambda p: p)
    v_core.wait()
    v1_s[...] = v0_s[:, :, c] + vc0_s[...]
    settle(w_x, wx_s, wm_s, nx)
    w_w = send(wm_s, wz_s, {"col_1": 1 - w})
    v_first = spread_to(v1_s, va_s, "row_1", y, ny, lambda p: (slice(None), p))

    lax.fori_loop(1 + nx // 2, nx + 1, query_side, 0)

    def copy_out(g):
        at = pl.ds(pl.multiple_of(8 * g, 8), 8)
        return pltpu.make_async_copy(pair_v.at[at], pair_out.at[at], out_sem.at[g])

    def pair_group(g, _):
        g_rows = g_s[tile(g, 128)]
        for b in range(8):
            rhs_s[128:256, 128 * b : 128 * (b + 1)] = pair_rows(g_rows, b)
        for b in range(4):
            two = mm(ab_s[:, tile(g, 256)], rhs_s[:, 256 * b : 256 * (b + 1)]).astype(BF16)
            pair_v[8 * g + 2 * b] = two[:, :128]
            pair_v[8 * g + 2 * b + 1] = two[:, 128:]
        copy_out(g).start()
        return 0

    lax.fori_loop(0, groups // 2, pair_group, 0)
    w_w.wait()
    wm_s[...] = wm_s[...] + wz_s[...]
    w_y = share(wm_s, wy_s, "row_1", y, ny)
    done(s_first)
    s2_s[...] = add([s1_s[z]] + [sa_s[r] for r in range(nz - 1)])
    s_second = spread_to(s2_s, sr_s, "row_1", y, ny, lambda p: p)
    done(v_first)
    v2_s[...] = add([v1_s[:, y]] + [va_s[r] for r in range(ny - 1)])
    v_second = spread_to(v2_s, vr_s, "row_0", z, nz, lambda p: p)
    done([q_copy(r) for r in range(1, nx)])
    qz_s[...] = add([qout_s[x]] + [qx_s[r] for r in range(nx - 1)])
    q_w = send(qz_s.at[1 - w], qr_s, {"col_1": 1 - w})
    settle(w_y, wy_s, wm_s, ny)
    w_z = share(wm_s, wr_s, "row_0", z, nz)
    lax.fori_loop(groups // 2, groups, pair_group, 0)
    done(s_second)
    kfin_ref[:, 0:F_ALL] = add([s2_s[y]] + [sr_s[r] for r in range(ny - 1)])
    done(v_second)
    kfin_ref[:, F_ALL:] = add([v2_s[z]] + [vr_s[r] for r in range(nz - 1)])
    q_w.wait()
    qfin_ref[...] = qz_s[w] + qr_s[...]
    settle(w_z, wr_s, wfin_ref, nz)
    for g in range(groups):
        copy_out(g).wait()


def finish(
    dims,
    pair_in,
    hw_ref,
    kfin_ref,
    qfin_ref,
    wfin_ref,
    qp_ref,
    kp_ref,
    vp_ref,
    rot_ref,
    tr_ref,
    gpt_ref,
    pair_out,
    q_out,
    qp_out,
    qf_out,
    k_out,
    v_out,
    kp_out,
    vp_out,
    kf_out,
    w_out,
    hw_out,
    t_s,
    pair_v,
    in_sem,
    out_sem,
):
    nz, ny, nx, ni, nj = dims
    z, y, c = lax.axis_index("row_0"), lax.axis_index("row_1"), lax.axis_index("row_2")
    x, w = lax.axis_index("col_0"), lax.axis_index("col_1")
    row = (z * ny + y) * 2 + c
    col = x * 2 + w
    slab = nj // (nz * ny * 2)
    qslab = ni // (nx * 2)

    groups = ni // 8

    def part(g, src, dst, sem):
        return pltpu.make_async_copy(src.at[pl.ds(8 * g, 8)], dst.at[pl.ds(8 * g, 8)], sem.at[g])

    for g in range(groups):
        part(g, pair_in, pair_v, in_sem).start()
    def exact(a, b):
        return jnp.dot(a, b, precision=HIGHEST)

    def from_lane(rows, at):
        return pltpu.roll(rows, lax.rem(128 - at, 128), 1)

    def over(t):
        return jnp.sum(t, axis=1, keepdims=True)

    def columns(t):
        return [[t[:, 3 * a + b : 3 * a + b + 1] for b in range(3)] for a in range(3)]

    def back(rot, v):
        return [rot[0][b] * v[0] + rot[1][b] * v[1] + rot[2][b] * v[2] for b in range(3)]

    def frame(out, cols, count):
        t = jnp.zeros((count, 128), F32)
        for n in range(12):
            t = jnp.where(iota((count, 128), 1) == n, cols[n // 4][n % 4], t)
        t_s[0:count] = t
        turned = jnp.transpose(t_s[0:128])
        for a in range(3):
            out[a] = turned[4 * a : 4 * a + 4, :count]

    expand = (iota((HP, 48), 0) == (iota((HP, 48), 1) >> 2)).astype(F32)
    coef = jnp.broadcast_to(coef_column(hw_ref, iota((48, 1), 0) >> 2), (48, 48))
    coef = jnp.where(iota((48, 48), 0) == iota((48, 48), 1), coef, 0.0)
    coef = jnp.sum(coef, axis=0, keepdims=True)

    t_s[...] = jnp.zeros(t_s.shape, F32)
    at = row * slab
    base = tile(col * (nj // 128) + at // 128, 128)
    here = tile(at // 128, 128)
    for a in range(3):
        t_s[3 * a : 3 * a + 3] = rot_ref[a, :, base]
        t_s[16 + 48 * a : 16 + 48 * (a + 1)] = kp_ref[a, :, here]
        t_s[160 + 96 * a : 160 + 96 * (a + 1)] = vp_ref[a, :, here]
    t_s[9:12] = tr_ref[:, base]
    own = jnp.transpose(from_lane(t_s[...], lax.rem(at, 128)))[:slab]
    rot = columns(own)
    shift = [own[:, 9 + a : 10 + a] for a in range(3)]
    kp = [own[:, 16 + 48 * b : 16 + 48 * (b + 1)] for b in range(3)]
    vp = [own[:, 160 + 96 * b : 160 + 96 * (b + 1)] for b in range(3)]
    kg = rotate(rot, kp, shift)
    k_out[...] = (WL * WS) * kfin_ref[:, 0:F_PT]
    v_out[...] = kfin_ref[:, F_ALL : F_ALL + G_PT]
    sums = exact(kfin_ref[:, F_N2 : F_N2 + HP], expand)
    dkg = []
    for a in range(3):
        piece = kfin_ref[:, F_PT + 48 * a : F_PT + 48 * (a + 1)]
        dkg.append(2.0 * coef * (piece - kg[a] * sums))
    v_at = F_ALL + G_PT
    dvg = [kfin_ref[:, v_at + 96 * a : v_at + 96 * (a + 1)] for a in range(3)]
    for b, (dk, dv) in enumerate(zip(back(rot, dkg), back(rot, dvg))):
        kp_out[b] = dk
        vp_out[b] = dv
    cols = []
    for a in range(3):
        cols.append([over(dkg[a] * kp[b]) + over(dvg[a] * vp[b]) for b in range(3)])
        cols[a].append(over(dkg[a]) + over(dvg[a]))
    frame(kf_out, cols, slab)

    for g in range(groups):
        part(g, pair_in, pair_v, in_sem).wait()
        part(g, pair_v, pair_out, out_sem).start()

    at = col * qslab
    base = tile(z * ny + y, 128)
    t_s[...] = jnp.zeros(t_s.shape, F32)
    for a in range(3):
        t_s[3 * a : 3 * a + 3] = rot_ref[a, :, base]
        t_s[16 + 48 * a : 16 + 48 * (a + 1), 0:ni] = qp_ref[a]
    t_s[9:12] = tr_ref[:, base]
    t_s[0:16] = from_lane(t_s[0:16], c * ni + at)
    t_s[16:160] = from_lane(t_s[16:160], at)
    own = jnp.transpose(t_s[0:256])[:qslab]
    rot = columns(own)
    shift = [own[:, 9 + a : 10 + a] for a in range(3)]
    qp = [own[:, 16 + 48 * b : 16 + 48 * (b + 1)] for b in range(3)]
    gp = [gpt_ref[b, tile(col, qslab), :] for b in range(3)]
    qg = rotate(rot, qp, shift)
    gg = rotate(rot, gp)
    q_out[...] = (WL * WS) * qfin_ref[:, 0:F_PT]
    sums = exact(qfin_ref[:, F_N1:F_N2], expand)
    dqg = []
    for a in range(3):
        piece = qfin_ref[:, F_PT + 48 * a : F_PT + 48 * (a + 1)]
        dqg.append(-2.0 * coef * (qg[a] * sums - piece))
    opt = [qfin_ref[:, F_N2 + 96 * a : F_N2 + 96 * (a + 1)] - shift[a] for a in range(3)]
    for b, dq in enumerate(back(rot, dqg)):
        qp_out[b] = dq
    cols = []
    for a in range(3):
        cols.append([over(dqg[a] * qp[b]) + over(opt[a] * gp[b]) for b in range(3)])
        cols[a].append(over(dqg[a]) - over(gg[a]))
    frame(qf_out, cols, qslab)

    w_out[...] = wfin_ref[0:H]
    total = jnp.zeros((1, 128), F32)
    for n in range(2):
        f = iota((128, 128), 0) + 128 * (n + 1)
        keep = (head_of_feature(f) == iota((128, 128), 1)) & (f >= F_PT)
        total += exact(wfin_ref[H + n : H + n + 1], keep.astype(F32))
    hw = hw_ref[...]
    hw_out[...] = total[:, 0:H] / (softplus(hw) * (1.0 + jnp.exp(-hw)))

    for g in range(groups):
        part(g, pair_v, pair_out, out_sem).wait()


def per_device(dims, *args):
    (pair, bw, hw, q, k, v, qp, kp, vp, rot, tr, count, go, gpt, gpair) = args
    nz, ny, nx, ni, nj = dims
    hw = hw.reshape(1, H)
    bw, q, go = bw.T, q.T, go.T
    gpt = jnp.transpose(gpt, (0, 2, 1))
    gpair = jnp.transpose(gpair, (1, 0, 2))
    lanes = ni * HP
    slab, qslab = nj // (nz * ny * 2), ni // (nx * 2)
    kw, qw = F_ALL + G_ALL, F_N2 + G_END - G_PT
    groups = lanes // 128
    sends = 3 * nx + 3 * (ny - 1) + 3 * (nz - 1) + 3

    def buf(*shape, dtype=F32):
        return pltpu.VMEM(shape, dtype)

    pair_grad, kfin, qfin, wfin = pl.pallas_call(
        functools.partial(mega, dims),
        out_shape=[
            jax.ShapeDtypeStruct((ni, nj, CZ), BF16),
            jax.ShapeDtypeStruct((slab, kw), F32),
            jax.ShapeDtypeStruct((qslab, qw), F32),
            jax.ShapeDtypeStruct((HP, 128), F32),
        ],
        in_specs=[ANY] + [VMEM] * 10 + [SMEM] + [VMEM] * 3,
        out_specs=[ANY] + [VMEM] * 3,
        scratch_shapes=[
            buf(ni, nj, CZ, dtype=BF16),
            buf(F_ALL, ni),
            buf(F_ALL, nj),
            buf(G_ALL, nj),
            buf(G_ALL, ni),
            buf(nj, F_ALL),
            buf(nj, 6 * F_ALL, dtype=BF16),
            buf(6 * F_ALL, lanes, dtype=BF16),
            buf(nj, 3 * G_ALL, dtype=BF16),
            buf(3 * G_ALL, lanes, dtype=BF16),
            buf(2, F_ALL, nj, dtype=BF16),
            buf(2, G_END - G_PT, nj, dtype=BF16),
            buf(HP, 128),
            buf(lanes, 128),
            buf(nj, lanes),
            buf(nj, lanes),
            buf(2, nj, 256),
            buf(nj, 2 * lanes, dtype=BF16),
            buf(256, 1024, dtype=BF16),
            buf(nj, lanes, dtype=BF16),
            buf(nj, lanes, dtype=BF16),
            buf(nj, lanes, dtype=BF16),
            buf(nj, lanes, dtype=BF16),
            buf(nx, 2, qslab, qw),
            buf(3, groups, 128),
            buf(nx - 1, 3, groups, 128),
            buf(3, groups, 128),
            buf(3, groups, 128),
            buf(2, groups, 128),
            buf(nz, ny, 2, slab, F_ALL),
            buf(nz, ny, slab, F_ALL),
            buf(nz, ny, slab, F_ALL),
            buf(nz - 1, ny, slab, F_ALL),
            buf(ny, slab, F_ALL),
            buf(ny - 1, slab, F_ALL),
            buf(nz, ny, 2, slab, G_ALL),
            buf(nz, ny, slab, G_ALL),
            buf(nz, ny, slab, G_ALL),
            buf(ny - 1, nz, slab, G_ALL),
            buf(nz, slab, G_ALL),
            buf(nz - 1, slab, G_ALL),
            buf(nx - 1, 2, qslab, qw),
            buf(2, qslab, qw),
            buf(qslab, qw),
            buf(HP, 128),
            buf(nx, HP, 128),
            buf(HP, 128),
            buf(HP, 128),
            buf(ny, HP, 128),
            buf(nz, HP, 128),
            pltpu.SemaphoreType.DMA((groups,)),
            pltpu.SemaphoreType.DMA((groups,)),
            pltpu.SemaphoreType.DMA((sends,)),
            pltpu.SemaphoreType.DMA((sends,)),
        ],
        compiler_params=pltpu.CompilerParams(
            collective_id=0, has_side_effects=True, vmem_limit_bytes=60 * 2**20
        ),
        name="tile_and_reduce",
    )(pair, bw, hw, q, k, v, qp, kp, vp, rot, tr, count, go, gpt, gpair)

    outs = [
        jax.ShapeDtypeStruct((ni, nj, CZ), BF16),
        jax.ShapeDtypeStruct((qslab, H * C), F32),
        jax.ShapeDtypeStruct((3, qslab, H * PQ), F32),
        jax.ShapeDtypeStruct((3, 4, qslab), F32),
        jax.ShapeDtypeStruct((slab, H * C), F32),
        jax.ShapeDtypeStruct((slab, H * C), F32),
        jax.ShapeDtypeStruct((3, slab, H * PQ), F32),
        jax.ShapeDtypeStruct((3, slab, H * PV), F32),
        jax.ShapeDtypeStruct((3, 4, slab), F32),
        jax.ShapeDtypeStruct((H, CZ), F32),
        jax.ShapeDtypeStruct((1, H), F32),
    ]
    small = [hw, kfin, qfin, wfin, qp, kp, vp, rot, tr, gpt]
    res = pl.pallas_call(
        functools.partial(finish, dims),
        out_shape=outs,
        in_specs=[ANY] + [VMEM] * 10,
        out_specs=[ANY] + [VMEM] * 10,
        scratch_shapes=[
            buf(512, 128),
            buf(ni, nj, CZ, dtype=BF16),
            pltpu.SemaphoreType.DMA((groups,)),
            pltpu.SemaphoreType.DMA((groups,)),
        ],
        compiler_params=pltpu.CompilerParams(vmem_limit_bytes=60 * 2**20),
        name="pair_and_frames",
    )(pair_grad, *small)
    pair_grad, dq, dqp, dqf, dk, dv, dkp, dvp, dkf, dw, dhw = res
    turn = functools.partial(jnp.transpose, axes=(0, 2, 1))
    return pair_grad, dq.T, turn(dqp), dqf, dk.T, dv.T, turn(dkp), turn(dvp), dkf, dw.T, dhw[0]


def solution(mesh):
    finer = Mesh(mesh.devices.reshape(4, 4, 2, 4, 2), ("row_0", "row_1", "row_2", "col_0", "col_1"))
    return sharded(finer, 64, 256)


def sharded(finer, ni, nj):
    sizes = finer.shape
    dims = (sizes["row_0"], sizes["row_1"], sizes["col_0"], ni, nj)
    in_specs = (
        P(ROW, COL, None),
        P(),
        P(),
        P(None, ROW),
        P(None, COL),
        P(None, COL),
        P(None, None, ROW),
        P(None, None, COL),
        P(None, None, COL),
        P(),
        P(),
        P(),
        P(None, ROW),
        P(None, None, ROW),
        P(ROW, None, None),
    )
    out_specs = (
        P(ROW, COL, None),
        P(None, ROW_COL),
        P(None, None, ROW_COL),
        P(None, None, ROW_COL),
        P(None, COL_ROW),
        P(None, COL_ROW),
        P(None, None, COL_ROW),
        P(None, None, COL_ROW),
        P(None, None, COL_ROW),
        P(),
        P(),
    )
    return jax.shard_map(
        functools.partial(per_device, dims),
        mesh=finer,
        in_specs=in_specs,
        out_specs=out_specs,
        check_vma=False,
    )
```

```python
import functools
import math

import jax
import jax.numpy as jnp
from jax import lax
from jax.experimental import pallas as pl
from jax.experimental.pallas import tpu as pltpu
from jax.sharding import Mesh
from jax.sharding import PartitionSpec as P

ROW = ("row_0", "row_1", "row_2")
COL = ("col_0", "col_1")
ROW_COL = ("row_0", "row_1", "row_2", "col_0", "col_1")
COL_ROW = ("col_0", "col_1", "row_0", "row_1", "row_2")

MESH = pl.DeviceIdType.MESH
HIGHEST = lax.Precision.HIGHEST
F32 = jnp.float32
BF16 = jnp.bfloat16
VMEM = pl.BlockSpec(memory_space=pltpu.VMEM)
ANY = pl.BlockSpec(memory_space=pl.ANY)
SMEM = pl.BlockSpec(memory_space=pltpu.SMEM)

H, C, PQ, PV, CZ = 12, 16, 4, 8, 128
HP = 16
WL = math.sqrt(1.0 / 3.0)
WC = math.sqrt(2.0 / (9.0 * PQ))
WS = 1.0 / math.sqrt(C)

F_PT = H * C
F_N1 = F_PT + 3 * H * PQ
F_N2 = F_N1 + HP
F_ALL = 384
G_PT = H * C
G_END = G_PT + 3 * H * PV
G_ALL = 512


def iota(shape, dim):
    return lax.broadcasted_iota(jnp.int32, shape, dim)


def head_of_feature(r):
    t = r - F_PT
    t = jnp.where(t >= 96, t - 96, jnp.where(t >= 48, t - 48, t))
    head = jnp.where(r < F_PT, r >> 4, t >> 2)
    head = jnp.where(r >= F_N1, r - F_N1, head)
    head = jnp.where(r >= F_N2, r - F_N2, head)
    return jnp.where(r >= F_N2 + HP, 99, head)


def head_of_value_feature(r):
    t = r - G_PT
    t = jnp.where(t >= 192, t - 192, jnp.where(t >= 96, t - 96, t))
    head = jnp.where(r < G_PT, r >> 4, t >> 3)
    return jnp.where(r >= G_END, 99, head)


def split2(x):
    hi = x.astype(BF16)
    return hi, (x - hi.astype(F32)).astype(BF16)


def split3(x):
    hi = x.astype(BF16)
    rest = x - hi.astype(F32)
    mid = rest.astype(BF16)
    return hi, mid, (rest - mid.astype(F32)).astype(BF16)


def mm(a, b):
    return jnp.dot(a, b, preferred_element_type=F32)


def mm_nt(a, b):
    return lax.dot_general(a, b, (((1,), (1,)), ((), ())), preferred_element_type=F32)


def softplus(x):
    return jnp.maximum(x, 0.0) + jnp.log(1.0 + jnp.exp(-jnp.abs(x)))


def coef_column(hw_ref, heads):
    coef = (0.5 * WL * WC) * softplus(hw_ref[...])
    rows = heads.shape[0]
    return jnp.sum(
        jnp.where(heads == iota((rows, H), 1), jnp.broadcast_to(coef, (rows, H)), 0.0),
        axis=1,
        keepdims=True,
    )


def rotate(rot, local, shift=None):
    out = []
    for x in range(3):
        t = rot[x][0] * local[0] + rot[x][1] * local[1] + rot[x][2] * local[2]
        out.append(t if shift is None else t + shift[x])
    return out


def pair_rows(head_rows, lane_block):
    keep = (iota(head_rows.shape, 0) >> 4) == lane_block
    return jnp.where(keep, head_rows, 0.0).astype(BF16)


def tile(k, size):
    return pl.ds(pl.multiple_of(k * size, size), size)


def mega(
    dims,
    pair_hbm,
    bw_ref,
    hw_ref,
    q_ref,
    k_ref,
    v_ref,
    qp_ref,
    kp_ref,
    vp_ref,
    rot_ref,
    tr_ref,
    count_ref,
    go_ref,
    gpt_ref,
    gpair_ref,
    pair_out,
    kfin_ref,
    qfin_ref,
    wfin_ref,
    pair_v,
    qf_s,
    kf_s,
    vf_s,
    gf_s,
    kt_s,
    kcat_s,
    qcat_s,
    vcat_s,
    gcat_s,
    kparts_s,
    vparts_s,
    w_s,
    g_s,
    p_s,
    pr_s,
    bias_s,
    ab_s,
    rhs_s,
    dh_s,
    dl_s,
    ah_s,
    al_s,
    qout_s,
    st_s,
    xst_s,
    cst_s,
    zst_s,
    sc_s,
    s0_s,
    sc0_s,
    s1_s,
    sa_s,
    s2_s,
    sr_s,
    v0_s,
    vc0_s,
    v1_s,
    va_s,
    v2_s,
    vr_s,
    qx_s,
    qz_s,
    qr_s,
    wm_s,
    wx_s,
    wz_s,
    wc_s,
    wy_s,
    wr_s,
    pair_sem,
    out_sem,
    send_sem,
    recv_sem,
):
    nz, ny, nx, ni, nj = dims
    lanes = ni * HP
    groups = lanes // 128
    chunks = lanes // 256
    z, y, c = lax.axis_index("row_0"), lax.axis_index("row_1"), lax.axis_index("row_2")
    x, w = lax.axis_index("col_0"), lax.axis_index("col_1")

    for g in range(groups):
        pltpu.make_async_copy(
            pair_hbm.at[pl.ds(8 * g, 8)], pair_v.at[pl.ds(8 * g, 8)], pair_sem.at[g]
        ).start()

    barrier = pltpu.get_barrier_semaphore()
    peers = [{"row_2": 1 - c}, {"col_1": 1 - w}]
    peers += [{"row_1": lax.rem(y + r, ny)} for r in range(1, ny)]
    peers += [{"row_0": lax.rem(z + r, nz)} for r in range(1, nz)]
    peers += [{"col_0": lax.rem(x + r, nx)} for r in range(1, nx)]
    for peer in peers:
        pl.semaphore_signal(barrier, inc=1, device_id=peer, device_id_type=MESH)

    used = [0]

    def send(src, dst, peer):
        n = used[0]
        used[0] += 1
        copy = pltpu.make_async_remote_copy(
            src_ref=src,
            dst_ref=dst,
            send_sem=send_sem.at[n],
            recv_sem=recv_sem.at[n],
            device_id=peer,
            device_id_type=MESH,
        )
        copy.start()
        return copy

    base = pl.multiple_of((z * ny + y) * 128, 128)

    def own_half(full):
        return jnp.where(c == 1, pltpu.roll(full, 64, 1), full)[:, :ni]

    rot_q = []
    for a in range(3):
        t = own_half(rot_ref[a, :, pl.ds(base, 128)])
        rot_q.append([t[b : b + 1] for b in range(3)])
    t = own_half(tr_ref[:, pl.ds(base, 128)])
    tr_q = [t[a : a + 1] for a in range(3)]
    col = x * 2 + w
    kbase = tile(col, nj)
    rot_k = []
    for a in range(3):
        t = rot_ref[a, :, kbase]
        rot_k.append([t[b : b + 1] for b in range(3)])
    t = tr_ref[:, kbase]
    tr_k = [t[a : a + 1] for a in range(3)]

    norm_sel = ((iota((HP, 48), 1) >> 2) == iota((HP, 48), 0)).astype(F32)
    qg = rotate(rot_q, [qp_ref[b] for b in range(3)], tr_q)
    gg = rotate(rot_q, [jnp.transpose(gpt_ref[b]) for b in range(3)])
    qf_s[0:F_PT] = jnp.transpose(q_ref[...])
    for a in range(3):
        qf_s[F_PT + 48 * a : F_PT + 48 * (a + 1)] = qg[a]
    qf_s[F_N2 : F_N2 + HP] = jnp.ones((HP, ni), F32)
    qf_s[F_N1:F_N2] = jnp.dot(
        norm_sel, qg[0] * qg[0] + qg[1] * qg[1] + qg[2] * qg[2], precision=HIGHEST
    )
    qf_s[F_N2 + HP :] = jnp.zeros((F_ALL - F_N2 - HP, ni), F32)
    gf_s[0:G_PT] = jnp.transpose(go_ref[...])
    for a in range(3):
        gf_s[G_PT + 96 * a : G_PT + 96 * (a + 1)] = gg[a]
    gf_s[G_END:] = jnp.zeros((G_ALL - G_END, ni), F32)

    kg = rotate(rot_k, [kp_ref[b] for b in range(3)], tr_k)
    vg = rotate(rot_k, [vp_ref[b] for b in range(3)], tr_k)
    kf_s[0:F_PT] = k_ref[...]
    for a in range(3):
        kf_s[F_PT + 48 * a : F_PT + 48 * (a + 1)] = kg[a]
    kf_s[F_N2 : F_N2 + HP] = jnp.dot(
        norm_sel, kg[0] * kg[0] + kg[1] * kg[1] + kg[2] * kg[2], precision=HIGHEST
    )
    kf_s[F_N1:F_N2] = jnp.ones((HP, nj), F32)
    kf_s[F_N2 + HP :] = jnp.zeros((F_ALL - F_N2 - HP, nj), F32)
    vf_s[0:G_PT] = v_ref[...]
    for a in range(3):
        vf_s[G_PT + 96 * a : G_PT + 96 * (a + 1)] = vg[a]
    vf_s[G_END:] = jnp.zeros((G_ALL - G_END, nj), F32)

    r = iota((F_ALL, 1), 0)
    coef = coef_column(hw_ref, head_of_feature(r))
    scale = jnp.where(r < F_PT, WL * WS, jnp.where(r < F_N1, 2.0 * coef, -coef))
    kt = jnp.transpose(kf_s[...] * scale)
    kt_s[...] = kt
    hi, mid, lo = split3(kt)
    for n, part in enumerate((hi, hi, mid, mid, hi, lo)):
        kcat_s[:, F_ALL * n : F_ALL * (n + 1)] = part
    hi, lo = split2(jnp.transpose(vf_s[...]))
    for n, part in enumerate((hi, hi, lo)):
        vcat_s[:, G_ALL * n : G_ALL * (n + 1)] = part
    kparts_s[0], kparts_s[1] = split2(kf_s[...])
    vparts_s[0], vparts_s[1] = split2(vf_s[G_PT:G_END])

    q_parts = split3(qf_s[...])
    g_parts = split2(gf_s[...])

    def expand(n, _):
        lane = iota((ni, 256), 1)
        e = ((lane >> 4) + n * 16 == iota((ni, 256), 0)).astype(BF16)
        for b in range(F_ALL // 128):
            head = head_of_feature(iota((128, 256), 0) + 128 * b)
            keep = head == (iota((128, 256), 1) & 15)
            hi, mid, lo = [
                jnp.where(keep, mm(part[128 * b : 128 * (b + 1)], e), 0.0).astype(BF16)
                for part in q_parts
            ]
            for m, part in enumerate((hi, mid, hi, mid, lo, hi)):
                at = F_ALL * m + 128 * b
                qcat_s[at : at + 128, tile(n, 256)] = part
        for b in range(G_ALL // 128):
            head = head_of_value_feature(iota((128, 256), 0) + 128 * b)
            keep = head == (iota((128, 256), 1) & 15)
            hi, lo = [
                jnp.where(keep, mm(part[128 * b : 128 * (b + 1)], e), 0.0).astype(BF16)
                for part in g_parts
            ]
            for m, part in enumerate((hi, lo, hi)):
                at = G_ALL * m + 128 * b
                gcat_s[at : at + 128, tile(n, 256)] = part
        return 0

    lax.fori_loop(0, chunks, expand, 0)

    w_s[...] = jnp.zeros((HP, 128), F32)
    w_s[0:H] = bw_ref[...].astype(F32)
    g_s[...] = jnp.zeros((lanes, 128), F32)
    for b in range(H):
        g_s[pl.ds(b, ni, stride=HP), :] = gpair_ref[b].astype(F32)
    w_rows = jnp.concatenate([w_s[...]] * 8, axis=0)
    for b in range(8):
        rhs_s[0:128, 128 * b : 128 * (b + 1)] = pair_rows(w_rows, b)

    count = count_ref[0]

    def forward(n, _):
        t = tile(n, 256)
        p_s[:, t] = mm(kcat_s[...], qcat_s[:, t])
        pr_s[:, t] = mm(vcat_s[...], gcat_s[:, t])
        for half in range(2):
            g = 2 * n + half
            pltpu.make_async_copy(
                pair_hbm.at[pl.ds(8 * g, 8)], pair_v.at[pl.ds(8 * g, 8)], pair_sem.at[g]
            ).wait()
            g_rows = g_s[tile(g, 128)]
            for b in range(8):
                rhs_s[128:256, 128 * b : 128 * (b + 1)] = pair_rows(g_rows, b)
            acc = None
            for b in range(4):
                two = jnp.concatenate([pair_v[8 * g + 2 * b], pair_v[8 * g + 2 * b + 1]], axis=1)
                part = mm_nt(two, rhs_s[:, 256 * b : 256 * (b + 1)])
                acc = part if acc is None else acc + part
            bias_s[half] = acc
        first = col * nj
        peak = jnp.full((8, 256), -jnp.inf, F32)
        for b in range(0, nj, 32):
            rows = slice(b, b + 32)
            bias = jnp.concatenate([bias_s[0, rows, :128], bias_s[1, rows, :128]], axis=1)
            logits = p_s[rows, t] + WL * bias
            logits = jnp.where(iota((32, 256), 0) + (first + b) < count, logits, -1000000000.0)
            p_s[rows, t] = logits
            peak = jnp.maximum(peak, jnp.max(logits.reshape(4, 8, 256), axis=0))
        peak = jnp.max(peak, axis=0, keepdims=True)
        total = jnp.zeros((8, 256), F32)
        upper = jnp.zeros((8, 256), F32)
        for b in range(0, nj, 32):
            rows = slice(b, b + 32)
            more = jnp.concatenate([bias_s[0, rows, 128:], bias_s[1, rows, 128:]], axis=1)
            prod = pr_s[rows, t] + more
            e = jnp.exp(p_s[rows, t] - peak)
            pr_s[rows, t] = prod
            p_s[rows, t] = e
            total += jnp.sum(e.reshape(4, 8, 256), axis=0)
            upper += jnp.sum((e * prod).reshape(4, 8, 256), axis=0)
        total = jnp.sum(total, axis=0, keepdims=True)
        upper = jnp.sum(upper, axis=0, keepdims=True)
        for half in range(2):
            at = slice(128 * half, 128 * (half + 1))
            st_s[0, pl.ds(2 * n + half, 1), :] = peak[:, at]
            st_s[1, pl.ds(2 * n + half, 1), :] = total[:, at]
            st_s[2, pl.ds(2 * n + half, 1), :] = upper[:, at]
        return 0

    lax.fori_loop(0, chunks, forward, 0)

    pl.semaphore_wait(barrier, len(peers))
    copies = [send(st_s, xst_s.at[r - 1], {"col_0": lax.rem(x + r, nx)}) for r in range(1, nx)]
    for copy in copies:
        copy.wait()
    sets = [(st_s[0], st_s[1], st_s[2])]
    sets += [(xst_s[r, 0], xst_s[r, 1], xst_s[r, 2]) for r in range(nx - 1)]

    def merge(sets):
        peak = functools.reduce(jnp.maximum, [s[0] for s in sets])
        weights = [jnp.exp(s[0] - peak) for s in sets]
        total = sum(s[1] * f for s, f in zip(sets, weights))
        upper = sum(s[2] * f for s, f in zip(sets, weights))
        return peak, total, upper

    mine = merge(sets)
    for a in range(3):
        cst_s[a] = mine[a]
    send(cst_s, zst_s, {"col_1": 1 - w}).wait()
    peak, total, upper = merge([mine, (zst_s[0], zst_s[1], zst_s[2])])
    sc_s[0] = jnp.exp(st_s[0] - peak) / total
    sc_s[1] = upper / total

    def weights_of(g, acc):
        attn = p_s[:, tile(g, 128)] * sc_s[0, pl.ds(g, 1), :]
        dlog = attn * (pr_s[:, tile(g, 128)] - sc_s[1, pl.ds(g, 1), :])
        dh_s[:, tile(g, 128)], dl_s[:, tile(g, 128)] = split2(dlog)
        a_hi, a_lo = split2(attn)
        ah_s[:, tile(g, 128)] = a_hi
        al_s[:, tile(g, 128)] = a_lo
        scaled = WL * dlog
        ab_s[:, pl.ds(pl.multiple_of(g * 256, 256), 128)] = scaled.astype(BF16)
        ab_s[:, pl.ds(pl.multiple_of(g * 256 + 128, 128), 128)] = a_hi
        turned = jnp.transpose(dlog).astype(BF16)
        for b in range(8):
            acc = acc + mm(turned[16 * b : 16 * (b + 1)], pair_v[8 * g + b])
        return acc

    weight = lax.fori_loop(0, groups, weights_of, jnp.zeros((HP, 128), F32))

    slab = nj // (nz * ny * 2)

    def add(terms):
        return functools.reduce(lambda a, b: a + b, terms)

    def spread_to(src, dst, axis, me, count, slot):
        out = []
        for r in range(1, count):
            peer = lax.rem(me + r, count)
            out.append(send(src.at[slot(peer)], dst.at[r - 1], {axis: peer}))
        return out

    def done(copies):
        for copy in copies:
            copy.wait()

    kout = mm_nt(dh_s[...], qcat_s[0:F_ALL])
    kout += mm_nt(dh_s[...], qcat_s[F_ALL : 2 * F_ALL])
    kout += mm_nt(dl_s[...], qcat_s[0:F_ALL])
    s0_s[...] = kout.reshape(s0_s.shape)
    s_core = send(s0_s.at[:, :, 1 - c], sc0_s, {"row_2": 1 - c})
    spread = jnp.sum(kt_s[...] * kout, axis=0, keepdims=True)

    wm_s[0:H] = WL * weight[0:H]
    wm_s[H : H + 1] = spread[:, 128:256]
    wm_s[H + 1 : H + 2] = spread[:, 256:384]
    wm_s[H + 2 :] = jnp.zeros((HP - H - 2, 128), F32)

    def share(src, slots, axis, me, count):
        slots[me] = src[...]
        return [send(src, slots.at[me], {axis: lax.rem(me + r, count)}) for r in range(1, count)]

    def settle(copies, slots, dst, count):
        done(copies)
        dst[...] = add([slots[n] for n in range(count)])

    w_c = send(wm_s, wc_s, {"row_2": 1 - c})

    aout = mm_nt(ah_s[...], gcat_s[0:G_ALL])
    aout += mm_nt(ah_s[...], gcat_s[G_ALL : 2 * G_ALL])
    aout += mm_nt(al_s[...], gcat_s[0:G_ALL])
    v0_s[...] = aout.reshape(v0_s.shape)
    v_core = send(v0_s.at[:, :, 1 - c], vc0_s, {"row_2": 1 - c})

    w_c.wait()
    wm_s[...] = wm_s[...] + wc_s[...]
    w_x = share(wm_s, wx_s, "col_0", x, nx)
    qslab = ni // (nx * 2)
    first = used[0]
    used[0] += nx - 1

    def q_copy(r):
        peer = lax.rem(x + r, nx)
        return pltpu.make_async_remote_copy(
            src_ref=qout_s.at[peer],
            dst_ref=qx_s.at[r - 1],
            send_sem=send_sem.at[first + r - 1],
            recv_sem=recv_sem.at[first + r - 1],
            device_id={"col_0": peer},
            device_id_type=MESH,
        )

    def query_side(r, _):
        owner = lax.rem(x + r, nx)
        at = tile(owner, 256)
        e = ((iota((16, 256), 1) >> 4) == iota((16, 256), 0)).astype(BF16)
        his, los = [], []
        for parts, hi_ref, lo_ref, head_of, rows, start in (
            (kparts_s, dh_s, dl_s, head_of_feature, F_N2, 0),
            (vparts_s, ah_s, al_s, head_of_value_feature, G_END - G_PT, G_PT),
        ):
            full = mm(parts[0, 0:rows], hi_ref[:, at]) + mm(parts[0, 0:rows], lo_ref[:, at])
            full += mm(parts[1, 0:rows], hi_ref[:, at])
            keep = head_of(iota((rows, 256), 0) + start) == (iota((rows, 256), 1) & 15)
            hi, lo = split2(jnp.where(keep, full, 0.0))
            his.append(hi)
            los.append(lo)
        out = mm_nt(e, jnp.concatenate(his, axis=0)) + mm_nt(e, jnp.concatenate(los, axis=0))
        qout_s[owner] = out.reshape(2, qslab, qout_s.shape[3])

        @pl.when(r < nx)
        def _():
            q_copy(r).start()

        return 0

    lax.fori_loop(1, 1 + nx // 2, query_side, 0)
    s_core.wait()
    s1_s[...] = s0_s[:, :, c] + sc0_s[...]
    s_first = spread_to(s1_s, sa_s, "row_0", z, nz, lambda p: p)
    v_core.wait()
    v1_s[...] = v0_s[:, :, c] + vc0_s[...]
    v_first = spread_to(v1_s, va_s, "row_1", y, ny, lambda p: (slice(None), p))
    settle(w_x, wx_s, wm_s, nx)
    w_w = send(wm_s, wz_s, {"col_1": 1 - w})

    lax.fori_loop(1 + nx // 2, nx + 1, query_side, 0)

    def copy_out(g):
        at = pl.ds(pl.multiple_of(8 * g, 8), 8)
        return pltpu.make_async_copy(pair_v.at[at], pair_out.at[at], out_sem.at[g])

    def pair_group(g, _):
        g_rows = g_s[tile(g, 128)]
        for b in range(8):
            rhs_s[128:256, 128 * b : 128 * (b + 1)] = pair_rows(g_rows, b)
        for b in range(4):
            two = mm(ab_s[:, tile(g, 256)], rhs_s[:, 256 * b : 256 * (b + 1)]).astype(BF16)
            pair_v[8 * g + 2 * b] = two[:, :128]
            pair_v[8 * g + 2 * b + 1] = two[:, 128:]
        copy_out(g).start()
        return 0

    lax.fori_loop(0, groups // 2, pair_group, 0)
    w_w.wait()
    wm_s[...] = wm_s[...] + wz_s[...]
    w_y = share(wm_s, wy_s, "row_1", y, ny)
    done(s_first)
    s2_s[...] = add([s1_s[z]] + [sa_s[r] for r in range(nz - 1)])
    s_second = spread_to(s2_s, sr_s, "row_1", y, ny, lambda p: p)
    done(v_first)
    v2_s[...] = add([v1_s[:, y]] + [va_s[r] for r in range(ny - 1)])
    v_second = spread_to(v2_s, vr_s, "row_0", z, nz, lambda p: p)
    done([q_copy(r) for r in range(1, nx)])
    qz_s[...] = add([qout_s[x]] + [qx_s[r] for r in range(nx - 1)])
    q_w = send(qz_s.at[1 - w], qr_s, {"col_1": 1 - w})
    settle(w_y, wy_s, wm_s, ny)
    w_z = share(wm_s, wr_s, "row_0", z, nz)
    lax.fori_loop(groups // 2, groups, pair_group, 0)
    done(s_second)
    kfin_ref[:, 0:F_ALL] = add([s2_s[y]] + [sr_s[r] for r in range(ny - 1)])
    done(v_second)
    kfin_ref[:, F_ALL:] = add([v2_s[z]] + [vr_s[r] for r in range(nz - 1)])
    q_w.wait()
    qfin_ref[...] = qz_s[w] + qr_s[...]
    settle(w_z, wr_s, wfin_ref, nz)
    for g in range(groups):
        copy_out(g).wait()


def finish(
    dims,
    pair_in,
    hw_ref,
    kfin_ref,
    qfin_ref,
    wfin_ref,
    qp_ref,
    kp_ref,
    vp_ref,
    rot_ref,
    tr_ref,
    gpt_ref,
    pair_out,
    q_out,
    qp_out,
    qf_out,
    k_out,
    v_out,
    kp_out,
    vp_out,
    kf_out,
    w_out,
    hw_out,
    t_s,
    pair_v,
    in_sem,
    out_sem,
):
    nz, ny, nx, ni, nj = dims
    z, y, c = lax.axis_index("row_0"), lax.axis_index("row_1"), lax.axis_index("row_2")
    x, w = lax.axis_index("col_0"), lax.axis_index("col_1")
    row = (z * ny + y) * 2 + c
    col = x * 2 + w
    slab = nj // (nz * ny * 2)
    qslab = ni // (nx * 2)

    groups = ni // 8

    def part(g, src, dst, sem):
        return pltpu.make_async_copy(src.at[pl.ds(8 * g, 8)], dst.at[pl.ds(8 * g, 8)], sem.at[g])

    for g in range(groups):
        part(g, pair_in, pair_v, in_sem).start()
    def exact(a, b):
        return jnp.dot(a, b, precision=HIGHEST)

    def from_lane(rows, at):
        return pltpu.roll(rows, lax.rem(128 - at, 128), 1)

    def over(t):
        return jnp.sum(t, axis=1, keepdims=True)

    def columns(t):
        return [[t[:, 3 * a + b : 3 * a + b + 1] for b in range(3)] for a in range(3)]

    def back(rot, v):
        return [rot[0][b] * v[0] + rot[1][b] * v[1] + rot[2][b] * v[2] for b in range(3)]

    def frame(out, cols, count):
        t = jnp.zeros((count, 128), F32)
        for n in range(12):
            t = jnp.where(iota((count, 128), 1) == n, cols[n // 4][n % 4], t)
        t_s[0:count] = t
        turned = jnp.transpose(t_s[0:128])
        for a in range(3):
            out[a] = turned[4 * a : 4 * a + 4, :count]

    expand = (iota((HP, 48), 0) == (iota((HP, 48), 1) >> 2)).astype(F32)
    coef = jnp.broadcast_to(coef_column(hw_ref, iota((48, 1), 0) >> 2), (48, 48))
    coef = jnp.where(iota((48, 48), 0) == iota((48, 48), 1), coef, 0.0)
    coef = jnp.sum(coef, axis=0, keepdims=True)

    t_s[...] = jnp.zeros(t_s.shape, F32)
    at = row * slab
    base = tile(col * (nj // 128) + at // 128, 128)
    here = tile(at // 128, 128)
    for a in range(3):
        t_s[3 * a : 3 * a + 3] = rot_ref[a, :, base]
        t_s[16 + 48 * a : 16 + 48 * (a + 1)] = kp_ref[a, :, here]
        t_s[160 + 96 * a : 160 + 96 * (a + 1)] = vp_ref[a, :, here]
    t_s[9:12] = tr_ref[:, base]
    own = jnp.transpose(from_lane(t_s[...], lax.rem(at, 128)))[:slab]
    rot = columns(own)
    shift = [own[:, 9 + a : 10 + a] for a in range(3)]
    kp = [own[:, 16 + 48 * b : 16 + 48 * (b + 1)] for b in range(3)]
    vp = [own[:, 160 + 96 * b : 160 + 96 * (b + 1)] for b in range(3)]
    kg = rotate(rot, kp, shift)
    k_out[...] = (WL * WS) * kfin_ref[:, 0:F_PT]
    v_out[...] = kfin_ref[:, F_ALL : F_ALL + G_PT]
    sums = exact(kfin_ref[:, F_N2 : F_N2 + HP], expand)
    dkg = []
    for a in range(3):
        piece = kfin_ref[:, F_PT + 48 * a : F_PT + 48 * (a + 1)]
        dkg.append(2.0 * coef * (piece - kg[a] * sums))
    v_at = F_ALL + G_PT
    dvg = [kfin_ref[:, v_at + 96 * a : v_at + 96 * (a + 1)] for a in range(3)]
    for b, (dk, dv) in enumerate(zip(back(rot, dkg), back(rot, dvg))):
        kp_out[b] = dk
        vp_out[b] = dv
    cols = []
    for a in range(3):
        cols.append([over(dkg[a] * kp[b]) + over(dvg[a] * vp[b]) for b in range(3)])
        cols[a].append(over(dkg[a]) + over(dvg[a]))
    frame(kf_out, cols, slab)

    for g in range(groups):
        part(g, pair_in, pair_v, in_sem).wait()
        part(g, pair_v, pair_out, out_sem).start()

    at = col * qslab
    base = tile(z * ny + y, 128)
    t_s[...] = jnp.zeros(t_s.shape, F32)
    for a in range(3):
        t_s[3 * a : 3 * a + 3] = rot_ref[a, :, base]
        t_s[16 + 48 * a : 16 + 48 * (a + 1), 0:ni] = qp_ref[a]
    t_s[9:12] = tr_ref[:, base]
    t_s[0:16] = from_lane(t_s[0:16], c * ni + at)
    t_s[16:160] = from_lane(t_s[16:160], at)
    own = jnp.transpose(t_s[0:256])[:qslab]
    rot = columns(own)
    shift = [own[:, 9 + a : 10 + a] for a in range(3)]
    qp = [own[:, 16 + 48 * b : 16 + 48 * (b + 1)] for b in range(3)]
    gp = [gpt_ref[b, tile(col, qslab), :] for b in range(3)]
    qg = rotate(rot, qp, shift)
    gg = rotate(rot, gp)
    q_out[...] = (WL * WS) * qfin_ref[:, 0:F_PT]
    sums = exact(qfin_ref[:, F_N1:F_N2], expand)
    dqg = []
    for a in range(3):
        piece = qfin_ref[:, F_PT + 48 * a : F_PT + 48 * (a + 1)]
        dqg.append(-2.0 * coef * (qg[a] * sums - piece))
    opt = [qfin_ref[:, F_N2 + 96 * a : F_N2 + 96 * (a + 1)] - shift[a] for a in range(3)]
    for b, dq in enumerate(back(rot, dqg)):
        qp_out[b] = dq
    cols = []
    for a in range(3):
        cols.append([over(dqg[a] * qp[b]) + over(opt[a] * gp[b]) for b in range(3)])
        cols[a].append(over(dqg[a]) - over(gg[a]))
    frame(qf_out, cols, qslab)

    w_out[...] = wfin_ref[0:H]
    total = jnp.zeros((1, 128), F32)
    for n in range(2):
        f = iota((128, 128), 0) + 128 * (n + 1)
        keep = (head_of_feature(f) == iota((128, 128), 1)) & (f >= F_PT)
        total += exact(wfin_ref[H + n : H + n + 1], keep.astype(F32))
    hw = hw_ref[...]
    hw_out[...] = total[:, 0:H] / (softplus(hw) * (1.0 + jnp.exp(-hw)))

    for g in range(groups):
        part(g, pair_v, pair_out, out_sem).wait()


def per_device(dims, *args):
    (pair, bw, hw, q, k, v, qp, kp, vp, rot, tr, count, go, gpt, gpair) = args
    nz, ny, nx, ni, nj = dims
    hw = hw.reshape(1, H)
    bw, q, go = bw.T, q.T, go.T
    gpt = jnp.transpose(gpt, (0, 2, 1))
    gpair = jnp.transpose(gpair, (1, 0, 2))
    lanes = ni * HP
    slab, qslab = nj // (nz * ny * 2), ni // (nx * 2)
    kw, qw = F_ALL + G_ALL, F_N2 + G_END - G_PT
    groups = lanes // 128
    sends = 3 * nx + 3 * (ny - 1) + 3 * (nz - 1) + 3

    def buf(*shape, dtype=F32):
        return pltpu.VMEM(shape, dtype)

    pair_grad, kfin, qfin, wfin = pl.pallas_call(
        functools.partial(mega, dims),
        out_shape=[
            jax.ShapeDtypeStruct((ni, nj, CZ), BF16),
            jax.ShapeDtypeStruct((slab, kw), F32),
            jax.ShapeDtypeStruct((qslab, qw), F32),
            jax.ShapeDtypeStruct((HP, 128), F32),
        ],
        in_specs=[ANY] + [VMEM] * 10 + [SMEM] + [VMEM] * 3,
        out_specs=[ANY] + [VMEM] * 3,
        scratch_shapes=[
            buf(ni, nj, CZ, dtype=BF16),
            buf(F_ALL, ni),
            buf(F_ALL, nj),
            buf(G_ALL, nj),
            buf(G_ALL, ni),
            buf(nj, F_ALL),
            buf(nj, 6 * F_ALL, dtype=BF16),
            buf(6 * F_ALL, lanes, dtype=BF16),
            buf(nj, 3 * G_ALL, dtype=BF16),
            buf(3 * G_ALL, lanes, dtype=BF16),
            buf(2, F_ALL, nj, dtype=BF16),
            buf(2, G_END - G_PT, nj, dtype=BF16),
            buf(HP, 128),
            buf(lanes, 128),
            buf(nj, lanes),
            buf(nj, lanes),
            buf(2, nj, 256),
            buf(nj, 2 * lanes, dtype=BF16),
            buf(256, 1024, dtype=BF16),
            buf(nj, lanes, dtype=BF16),
            buf(nj, lanes, dtype=BF16),
            buf(nj, lanes, dtype=BF16),
            buf(nj, lanes, dtype=BF16),
            buf(nx, 2, qslab, qw),
            buf(3, groups, 128),
            buf(nx - 1, 3, groups, 128),
            buf(3, groups, 128),
            buf(3, groups, 128),
            buf(2, groups, 128),
            buf(nz, ny, 2, slab, F_ALL),
            buf(nz, ny, slab, F_ALL),
            buf(nz, ny, slab, F_ALL),
            buf(nz - 1, ny, slab, F_ALL),
            buf(ny, slab, F_ALL),
            buf(ny - 1, slab, F_ALL),
            buf(nz, ny, 2, slab, G_ALL),
            buf(nz, ny, slab, G_ALL),
            buf(nz, ny, slab, G_ALL),
            buf(ny - 1, nz, slab, G_ALL),
            buf(nz, slab, G_ALL),
            buf(nz - 1, slab, G_ALL),
            buf(nx - 1, 2, qslab, qw),
            buf(2, qslab, qw),
            buf(qslab, qw),
            buf(HP, 128),
            buf(nx, HP, 128),
            buf(HP, 128),
            buf(HP, 128),
            buf(ny, HP, 128),
            buf(nz, HP, 128),
            pltpu.SemaphoreType.DMA((groups,)),
            pltpu.SemaphoreType.DMA((groups,)),
            pltpu.SemaphoreType.DMA((sends,)),
            pltpu.SemaphoreType.DMA((sends,)),
        ],
        compiler_params=pltpu.CompilerParams(
            collective_id=0, has_side_effects=True, vmem_limit_bytes=60 * 2**20
        ),
        name="tile_and_reduce",
    )(pair, bw, hw, q, k, v, qp, kp, vp, rot, tr, count, go, gpt, gpair)

    outs = [
        jax.ShapeDtypeStruct((ni, nj, CZ), BF16),
        jax.ShapeDtypeStruct((qslab, H * C), F32),
        jax.ShapeDtypeStruct((3, qslab, H * PQ), F32),
        jax.ShapeDtypeStruct((3, 4, qslab), F32),
        jax.ShapeDtypeStruct((slab, H * C), F32),
        jax.ShapeDtypeStruct((slab, H * C), F32),
        jax.ShapeDtypeStruct((3, slab, H * PQ), F32),
        jax.ShapeDtypeStruct((3, slab, H * PV), F32),
        jax.ShapeDtypeStruct((3, 4, slab), F32),
        jax.ShapeDtypeStruct((H, CZ), F32),
        jax.ShapeDtypeStruct((1, H), F32),
    ]
    small = [hw, kfin, qfin, wfin, qp, kp, vp, rot, tr, gpt]
    res = pl.pallas_call(
        functools.partial(finish, dims),
        out_shape=outs,
        in_specs=[ANY] + [VMEM] * 10,
        out_specs=[ANY] + [VMEM] * 10,
        scratch_shapes=[
            buf(512, 128),
            buf(ni, nj, CZ, dtype=BF16),
            pltpu.SemaphoreType.DMA((groups,)),
            pltpu.SemaphoreType.DMA((groups,)),
        ],
        compiler_params=pltpu.CompilerParams(vmem_limit_bytes=60 * 2**20),
        name="pair_and_frames",
    )(pair_grad, *small)
    pair_grad, dq, dqp, dqf, dk, dv, dkp, dvp, dkf, dw, dhw = res
    turn = functools.partial(jnp.transpose, axes=(0, 2, 1))
    return pair_grad, dq.T, turn(dqp), dqf, dk.T, dv.T, turn(dkp), turn(dvp), dkf, dw.T, dhw[0]


def solution(mesh):
    finer = Mesh(mesh.devices.reshape(4, 4, 2, 4, 2), ("row_0", "row_1", "row_2", "col_0", "col_1"))
    return sharded(finer, 64, 256)


def sharded(finer, ni, nj):
    sizes = finer.shape
    dims = (sizes["row_0"], sizes["row_1"], sizes["col_0"], ni, nj)
    in_specs = (
        P(ROW, COL, None),
        P(),
        P(),
        P(None, ROW),
        P(None, COL),
        P(None, COL),
        P(None, None, ROW),
        P(None, None, COL),
        P(None, None, COL),
        P(),
        P(),
        P(),
        P(None, ROW),
        P(None, None, ROW),
        P(ROW, None, None),
    )
    out_specs = (
        P(ROW, COL, None),
        P(None, ROW_COL),
        P(None, None, ROW_COL),
        P(None, None, ROW_COL),
        P(None, COL_ROW),
        P(None, COL_ROW),
        P(None, None, COL_ROW),
        P(None, None, COL_ROW),
        P(None, None, COL_ROW),
        P(),
        P(),
    )
    return jax.shard_map(
        functools.partial(per_device, dims),
        mesh=finer,
        in_specs=in_specs,
        out_specs=out_specs,
        check_vma=False,
    )
```
